256 devices in a mesh: gx: 32 (over x, z), gy: 8 (over y, core).
Axes of the slice: x: 4, y: 4, z: 8, core: 2. Of those that a mesh axis runs over, the one named last changes fastest.
Arguments:
- velocity_x: float32 [1024, 8, 384], P('gx', 'gy'), may hold values from -6 to 6
- velocity_z: float32 [1024, 8, 384], P('gx', 'gy'), may hold values from -6 to 6
- stress_xx: float32 [1024, 8, 384], P('gx', 'gy'), may hold values from -6 to 6
- stress_zz: float32 [1024, 8, 384], P('gx', 'gy'), may hold values from -6 to 6
- stress_xz: float32 [1024, 8, 384], P('gx', 'gy'), may hold values from -6 to 6
- material: int32 [1024, 8, 384], P('gx', 'gy'), may hold values from 0 to 15, as said below
- land_mask: int32 [1024, 8], P('gx', 'gy'), may hold values 0 or 1
- density: float32 [16], replicated, may hold values from 1 to 3
- lame_lambda: float32 [16], replicated, may hold values from 0.5 to 4
- shear_modulus: float32 [16], replicated, may hold values from 0.3 to 2
- continuation_land: float32 [26, 27], replicated, may hold values from -1.25 to 1.25
- continuation_sea: float32 [26, 27], replicated, may hold values from -1.25 to 1.25
- continuation_bottom: float32 [26, 27], replicated, may hold values from -1.25 to 1.25
Outputs:
- next_velocity_x: float32 [1024, 8, 384], P('gx', 'gy')
- next_velocity_z: float32 [1024, 8, 384], P('gx', 'gy')
- next_stress_xx: float32 [1024, 8, 384], P('gx', 'gy')
- next_stress_zz: float32 [1024, 8, 384], P('gx', 'gy')
- next_stress_xz: float32 [1024, 8, 384], P('gx', 'gy')
The draws below stay inside these ranges and needn't reach their ends.
Inputs may be any that keep to these rules, and one draw needn't show every extreme that they name: `material`: in every vertical line the layer number never falls with depth, and it is 0 at depth index 0.
All inputs are finite; a program needn't handle non-finite values. No bound on the sum of `land_mask` on one device may be relied on, other than what follows from the above.
Results may differ from the reference program's by a relative error of at most 0.000073.
Values sent between devices are 32-bit elements; how exact they have to be, the bound alone decides.
A program may use at most 64 MiB of HBM per device.

```python
import math
import jax
import jax.numpy as jnp
from jax import lax

NX = 1024
NZ = 384
LAYERS = 16
WINDOW = 27
CONT = 26
SECTIONS = 8


def draw_material(key, part):
    thickness = jax.random.randint(key, (LAYERS - 1, NX, SECTIONS), 1, 2 * NZ // LAYERS)
    levels = lax.broadcasted_iota(jnp.int32, (NX, SECTIONS, NZ), 2)
    interface = jnp.zeros((NX, SECTIONS), jnp.int32)
    strata = jnp.zeros((NX, SECTIONS, NZ), jnp.int32)
    for boundary_index in range(LAYERS - 1):
        interface = interface + thickness[boundary_index]
        strata = strata + (levels >= interface[:, :, None]).astype(jnp.int32)
    return strata


def plant(drawn, stream_key, smallest, largest):
    longest = drawn.shape.index(max(drawn.shape))
    spots = []
    for shift in (0, 1):
        where = [jax.random.randint(jax.random.fold_in(stream_key, axis), (), 0, length) for axis, length in enumerate(drawn.shape)]
        where[longest] = (where[longest] + shift) % drawn.shape[longest]
        spots.append(tuple(where))
    return drawn.at[spots[0]].set(smallest).at[spots[1]].set(largest)


def block_scale(key, extent, shards, smallest, top_value):
    factor_of, own = 1.0, jax.random.fold_in(key, 6)
    for dim, parts in shards:
        heights = jnp.exp(jax.random.uniform(jax.random.fold_in(own, dim), (parts,), jnp.float32, smallest / len(shards), top_value / len(shards)))
        factor_of = factor_of * jnp.repeat(heights, extent[dim] // parts).reshape([-1 if axis == dim else 1 for axis in range(len(extent))])
    return factor_of


def gaussian(own_key, dims, spread, most, cuts=(), held_as=jnp.bfloat16):
    entries = spread * jax.random.normal(own_key, dims, jnp.float32)
    if cuts:
        entries = entries * block_scale(own_key, dims, cuts, -0.22, 0.18)
    return jnp.clip(entries, -most, most).astype(held_as)


def setup_inputs(seed: int = 0) -> dict:
    key_list = jax.random.split(jax.random.key(seed), 14)
    velocity_x = gaussian(key_list[0], (NX, SECTIONS, NZ), 1.0, 6.0, ((0, 32), (1, 8)), jnp.float32)
    velocity_z = gaussian(key_list[1], (NX, SECTIONS, NZ), 1.0, 6.0, ((0, 32), (1, 8)), jnp.float32)
    stress_xx = gaussian(key_list[2], (NX, SECTIONS, NZ), 1.0, 6.0, ((0, 32), (1, 8)), jnp.float32)
    stress_zz = gaussian(key_list[3], (NX, SECTIONS, NZ), 1.0, 6.0, ((0, 32), (1, 8)), jnp.float32)
    stress_xz = gaussian(key_list[4], (NX, SECTIONS, NZ), 1.0, 6.0, ((0, 32), (1, 8)), jnp.float32)
    material = draw_material(jax.random.fold_in(key_list[13], 71), 0)
    land_mask = plant((jax.random.randint(key_list[6], (NX, SECTIONS), 0, 2) < 1).astype(jnp.int32), jax.random.fold_in(key_list[6], 1), 0, 1)
    density = jnp.clip(jnp.exp(jax.random.uniform(key_list[7], (LAYERS,), jnp.float32, math.log(1.0), math.log(3.0))), 1.0, 3.0)
    lame_lambda = jnp.clip(jnp.exp(jax.random.uniform(key_list[8], (LAYERS,), jnp.float32, math.log(0.5), math.log(4.0))), 0.5, 4.0)
    shear_modulus = jnp.clip(jnp.exp(jax.random.uniform(key_list[9], (LAYERS,), jnp.float32, math.log(0.3), math.log(2.0))), 0.3, 2.0)
    continuation_land = gaussian(key_list[10], (CONT, WINDOW), WINDOW ** -0.5, 1.25, (), jnp.float32)
    continuation_sea = gaussian(key_list[11], (CONT, WINDOW), WINDOW ** -0.5, 1.25, (), jnp.float32)
    continuation_bottom = gaussian(key_list[12], (CONT, WINDOW), WINDOW ** -0.5, 1.25, (), jnp.float32)
    return dict(velocity_x=velocity_x, velocity_z=velocity_z, stress_xx=stress_xx, stress_zz=stress_zz, stress_xz=stress_xz, material=material, land_mask=land_mask, density=density, lame_lambda=lame_lambda, shear_modulus=shear_modulus, continuation_land=continuation_land, continuation_sea=continuation_sea, continuation_bottom=continuation_bottom)


time_step = 0.2
highest = lax.Precision.HIGHEST


def spectral(length):
    indices = jnp.arange(length, dtype=jnp.int32)
    distance = jnp.mod(indices[:, None] - indices[None, :] + length // 2, length) - length // 2
    parity = 1.0 - 2.0 * jnp.mod(distance, 2).astype(jnp.float32)
    angles = jnp.pi * distance.astype(jnp.float32) / length
    tangent = jnp.where(distance == 0, 1.0, jnp.tan(angles))
    return jnp.where(distance == 0, 0.0, parity * (jnp.pi / length) / tangent)


def product(left, right):
    return jnp.dot(left, right, precision=highest, preferred_element_type=jnp.float32)


def reference(velocity_x, velocity_z, stress_xx, stress_zz, stress_xz, material, land_mask, density, lame_lambda, shear_modulus, continuation_land, continuation_sea, continuation_bottom):
    across_matrix = spectral(NX)
    depth_matrix = spectral(NZ + CONT)
    interior_t = depth_matrix[:NZ, :NZ].T
    boundary_t = depth_matrix[:NZ, NZ:].T
    land_rows = land_mask.reshape(-1, 1) > 0

    def lateral(quantity):
        return product(across_matrix, quantity.reshape(NX, -1)).reshape(quantity.shape)

    def vertical(quantity):
        lines = quantity.reshape(-1, NZ)
        upper = lines[:, :WINDOW]
        lower = lines[:, NZ - WINDOW:]
        extension = jnp.where(land_rows, product(upper, continuation_land.T), product(upper, continuation_sea.T)) + product(lower, continuation_bottom.T)
        return (product(lines, interior_t) + product(extension, boundary_t)).reshape(quantity.shape)

    buoyancy = 1.0 / density[material]
    lame_first = lame_lambda[material]
    shear_coef = shear_modulus[material]
    next_velocity_x = velocity_x + time_step * buoyancy * (lateral(stress_xx) + vertical(stress_xz))
    next_velocity_z = velocity_z + time_step * buoyancy * (lateral(stress_xz) + vertical(stress_zz))
    lateral_vx = lateral(next_velocity_x)
    lateral_vz = lateral(next_velocity_z)
    depth_vx = vertical(next_velocity_x)
    depth_vz = vertical(next_velocity_z)
    normal_coef = lame_first + 2.0 * shear_coef
    next_stress_xx = stress_xx + time_step * (normal_coef * lateral_vx + lame_first * depth_vz)
    next_stress_zz = stress_zz + time_step * (lame_first * lateral_vx + normal_coef * depth_vz)
    next_stress_xz = stress_xz + time_step * shear_coef * (depth_vx + lateral_vz)
    surface = lax.broadcasted_iota(jnp.int32, (1, 1, NZ), 2) == 0
    next_stress_zz = jnp.where(surface & (land_mask[:, :, None] > 0), 0.0, next_stress_zz)
    next_stress_xz = jnp.where(surface, 0.0, next_stress_xz)
    return next_velocity_x, next_velocity_z, next_stress_xx, next_stress_zz, next_stress_xz
```

```python
import functools

import jax
import jax.numpy as jnp
import numpy as np
from jax import lax
from jax.experimental import pallas as pl
from jax.experimental.pallas import tpu as pltpu
from jax.sharding import PartitionSpec as P

NX = 1024
NZ = 384
LAYERS = 16
WINDOW = 27
CONT = 26
RING_X = 4
RING_Z = 8
OWNERS = 32
ROWS = 12
CHUNK = 16
LANES = 128
TILES = 3
TIME_STEP = 0.2


def spectral(length):
    indices = np.arange(length)
    distance = np.mod(indices[:, None] - indices[None, :] + length // 2, length) - length // 2
    parity = 1.0 - 2.0 * np.mod(distance, 2)
    tangent = np.tan(np.pi * np.where(distance == 0, 1, distance) / length)
    return np.where(distance == 0, 0.0, parity * (np.pi / length) / tangent)


def two_parts(matrix):
    high = matrix.astype(np.float32).astype(jnp.bfloat16)
    low = (matrix.astype(np.float32) - high.astype(np.float32)).astype(jnp.bfloat16)
    return high, low


def parts_of(value):
    high = value.astype(jnp.bfloat16)
    low = (value - high.astype(jnp.float32)).astype(jnp.bfloat16)
    return high, low


def dot(left, right):
    return jnp.dot(left, right, preferred_element_type=jnp.float32)


def split_product(left, right_high, right_low):
    rows = left.shape[0]
    high, low = parts_of(left)
    both = dot(jnp.concatenate([high, low], axis=0), right_high)
    return both[:rows] + (both[rows:] + dot(high, right_low))


def swap_blocks(arrays):
    lane = lax.broadcasted_iota(jnp.int32, arrays[0].shape, 1)
    out = list(arrays)
    for bit, width in ((1, 32), (2, 64)):
        upper = (lane & width) != 0
        for k in range(4):
            if k & bit:
                continue
            first, second = out[k], out[k | bit]
            out[k] = jnp.where(upper, pltpu.roll(second, width, 1), first)
            out[k | bit] = jnp.where(upper, second, pltpu.roll(first, LANES - width, 1))
    return out


def lateral(fields, across_high, across_low):
    pairs = []
    for field in fields:
        blocks = field.reshape(4, 2, CHUNK, LANES)
        pairs.append(
            jnp.concatenate(
                [blocks[:, 0].reshape(64, LANES), blocks[:, 1].reshape(64, LANES)], axis=1
            )
        )
    spread = split_product(jnp.concatenate(pairs, axis=0), across_high, across_low)
    results = []
    for f in range(len(fields)):
        pieces = []
        for target in range(4):
            total = None
            for source in range(4):
                shift = (target - source) % 4
                row = 64 * f + CHUNK * source
                term = spread[row : row + CHUNK, 256 * shift : 256 * shift + 256]
                total = term if total is None else total + term
            pieces += [total[:, :LANES], total[:, LANES:]]
        results.append(jnp.concatenate(pieces, axis=0))
    return results


def vertical(lines, land, inner_high, inner_low, edge_high, edge_low):
    lane = lax.broadcasted_iota(jnp.int32, (lines.shape[0], LANES), 1)
    upper = jnp.where(lane < WINDOW, lines[:, :LANES], 0.0)
    lower = jnp.where(lane >= LANES - WINDOW, lines[:, NZ - LANES :], 0.0)
    edges = (
        jnp.where(land, upper, 0.0)
        + pltpu.roll(jnp.where(land, 0.0, upper), 32, 1)
        + pltpu.roll(lower, 64 + WINDOW, 1)
    )
    return split_product(lines, inner_high, inner_low) + split_product(edges, edge_high, edge_low)


def load_lines(ref):
    return jnp.concatenate([ref[pl.ds(t, 32, stride=TILES), :] for t in range(TILES)], axis=1)


def store_lines(ref, value):
    for t in range(TILES):
        ref[pl.ds(t, 32, stride=TILES), :] = value[:, LANES * t : LANES * (t + 1)]


def kernel(
    vx_hbm, vz_hbm, xx_hbm, zz_hbm, xz_hbm, material_hbm,
    land_ref, density_ref, lame_ref, shear_ref, gland_ref, gsea_ref, gbottom_ref, bound_ref,
    inner_high_hbm, inner_low_hbm, across_high_hbm, across_low_hbm,
    vx_out, vz_out, xx_out, zz_out, xz_out,
    vx_ref, vz_ref, xx_ref, zz_ref, xz_ref, material_ref,
    inner_high_ref, inner_low_ref, across_high_ref, across_low_ref,
    packed, outgoing, incoming, returned, home, load_sem,
    send_sem, recv_sem, send_back_sem, recv_back_sem,
):
    me = lax.axis_index("gx")
    my_x, my_z = me // RING_Z, me % RING_Z

    def offset(step):
        group = step // 4
        half = (group + 1) // 2
        dz = 4 + half * (1 - 2 * (group % 2))
        dx = (2 + (step % 4)) % 4
        return dx, dz

    def ahead(step):
        dx, dz = offset(step)
        return ((my_x + dx) % RING_X) * RING_Z + (my_z + dz) % RING_Z

    def behind(step):
        dx, dz = offset(step)
        return ((my_x + RING_X - dx) % RING_X) * RING_Z + (my_z + 2 * RING_Z - dz) % RING_Z

    def is_other(step):
        dx, dz = offset(step)
        return dx + (dz % RING_Z) != 0

    barrier = pltpu.get_barrier_semaphore()

    def greet(step, carry):
        @pl.when(is_other(step))
        def _():
            pl.semaphore_signal(barrier, inc=1, device_id={"gx": ahead(step)})

        return carry

    lax.fori_loop(0, OWNERS, greet, 0)

    pairs = (
        (material_hbm, material_ref), (xz_hbm, xz_ref), (zz_hbm, zz_ref),
        (inner_high_hbm, inner_high_ref), (inner_low_hbm, inner_low_ref),
        (vx_hbm, vx_ref), (vz_hbm, vz_ref), (xx_hbm, xx_ref),
        (across_high_hbm, across_high_ref), (across_low_hbm, across_low_ref),
    )
    loads = [pltpu.make_async_copy(a, b, load_sem.at[i]) for i, (a, b) in enumerate(pairs)]
    for load in loads:
        load.start()

    diagonal = lax.broadcasted_iota(jnp.int32, (32, 32), 0) == lax.broadcasted_iota(
        jnp.int32, (32, 32), 1
    )
    land = (
        jnp.sum(
            jnp.where(diagonal, jnp.broadcast_to(land_ref[...], (32, 32)), 0),
            axis=1,
            keepdims=True,
        )
        > 0
    )
    land_pair = jnp.broadcast_to(jnp.concatenate([land, land], axis=0), (64, LANES))

    gap = jnp.zeros((CONT, 32 - WINDOW), jnp.float32)
    grams = jnp.concatenate(
        [gland_ref[...], gap, gsea_ref[...], gap, gbottom_ref[...], gap,
         jnp.zeros((CONT, 32), jnp.float32)],
        axis=1,
    )
    folded = lax.dot_general(
        grams, bound_ref[...], (((0,), (0,)), ((), ())),
        precision=lax.Precision.HIGHEST, preferred_element_type=jnp.float32,
    )
    edge_high, edge_low = parts_of(folded)

    loads[0].wait()
    material = load_lines(material_ref)
    density = jnp.full(material.shape, density_ref[0], jnp.float32)
    lame = jnp.full(material.shape, lame_ref[0], jnp.float32)
    shear = jnp.full(material.shape, shear_ref[0], jnp.float32)
    for layer in range(1, LAYERS):
        chosen = material == layer
        density = jnp.where(chosen, density_ref[layer], density)
        lame = jnp.where(chosen, lame_ref[layer], lame)
        shear = jnp.where(chosen, shear_ref[layer], shear)
    light = TIME_STEP * (1.0 / density)

    for load in loads[1:5]:
        load.wait()
    inner_high, inner_low = inner_high_ref[...], inner_low_ref[...]
    stress_xz = load_lines(xz_ref)
    stress_zz = load_lines(zz_ref)
    depth = vertical(
        jnp.concatenate([stress_xz, stress_zz], axis=0), land_pair,
        inner_high, inner_low, edge_high, edge_low,
    )
    for load in loads[5:8]:
        load.wait()
    stress_xx = load_lines(xx_ref)
    part_vx = load_lines(vx_ref) + light * depth[:32]
    part_vz = load_lines(vz_ref) + light * depth[32:]

    packed[0] = jnp.concatenate([stress_xx, stress_xz, part_vx, part_vz], axis=0).T
    packed[1] = jnp.concatenate(
        [light] + [pltpu.roll(light, NZ - 3 * slot, 1) for slot in range(1, 4)], axis=0
    ).T
    for owner in range(OWNERS):
        outgoing[owner, :ROWS] = packed[0, ROWS * owner : ROWS * (owner + 1)]
        outgoing[owner, ROWS:] = packed[1, ROWS * owner : ROWS * owner + CHUNK - ROWS]
    incoming[me] = outgoing[me]

    pl.semaphore_wait(barrier, OWNERS - 1)

    def out_copy(step):
        return pltpu.make_async_remote_copy(
            src_ref=outgoing.at[ahead(step)], dst_ref=incoming.at[me],
            send_sem=send_sem.at[step], recv_sem=recv_sem.at[step],
            device_id={"gx": ahead(step)},
        )

    def in_copy(step):
        return pltpu.make_async_remote_copy(
            src_ref=outgoing.at[ahead(step)], dst_ref=incoming.at[behind(step)],
            send_sem=send_sem.at[step], recv_sem=recv_sem.at[step],
            device_id={"gx": ahead(step)},
        )

    def back_copy(step):
        return pltpu.make_async_remote_copy(
            src_ref=returned.at[ahead(step)], dst_ref=home.at[me],
            send_sem=send_back_sem.at[step], recv_sem=recv_back_sem.at[step],
            device_id={"gx": ahead(step)},
        )

    def home_copy(step):
        return pltpu.make_async_remote_copy(
            src_ref=returned.at[ahead(step)], dst_ref=home.at[behind(step)],
            send_sem=send_back_sem.at[step], recv_sem=recv_back_sem.at[step],
            device_id={"gx": ahead(step)},
        )

    def each_other(act):
        def step_of(step, carry):
            @pl.when(is_other(step))
            def _():
                act(step)

            return carry

        lax.fori_loop(0, OWNERS, step_of, 0)

    each_other(lambda step: out_copy(step).start())
    each_other(lambda step: in_copy(step).wait_recv())
    for load in loads[8:]:
        load.wait()
    across_high, across_low = across_high_ref[...], across_low_ref[...]

    got = incoming[...].reshape(8, 4, CHUNK, LANES)
    fields = swap_blocks([got[:, k].reshape(8 * CHUNK, LANES) for k in range(4)])
    row = lax.broadcasted_iota(jnp.int32, (8 * CHUNK, LANES), 0) % CHUNK
    factor = jnp.zeros((8 * CHUNK, LANES), jnp.float32)
    for slot in range(4):
        moved = pltpu.roll(fields[slot], 8 * CHUNK + 3 * slot - ROWS, 0)
        factor = jnp.where((row >= 3 * slot) & (row < 3 * slot + 3), moved, factor)
    slope = lateral(fields[:2], across_high, across_low)
    moved_vx = fields[2] + factor * slope[0]
    moved_vz = fields[3] + factor * slope[1]
    slope = lateral([moved_vx, moved_vz], across_high, across_low)
    back = swap_blocks([moved_vx, moved_vz, slope[0], slope[1]])
    for k in range(4):
        for group in range(8):
            returned[4 * group + k] = back[k][CHUNK * group : CHUNK * group + ROWS]
    home[me] = returned[me]

    each_other(lambda step: back_copy(step).start())
    each_other(lambda step: home_copy(step).wait_recv())

    for owner in range(OWNERS):
        packed[0, ROWS * owner : ROWS * (owner + 1)] = home[owner]
    settled = packed[0].T
    next_vx, next_vz = settled[:32], settled[32:64]
    lateral_vx, lateral_vz = settled[64:96], settled[96:]
    depth = vertical(
        settled[:64], land_pair, inner_high_ref[...], inner_low_ref[...], edge_high, edge_low
    )
    depth_vx, depth_vz = depth[:32], depth[32:]
    normal = lame + 2.0 * shear
    surface = lax.broadcasted_iota(jnp.int32, (32, NZ), 1) == 0
    next_xx = load_lines(xx_ref) + TIME_STEP * (normal * lateral_vx + lame * depth_vz)
    next_zz = load_lines(zz_ref) + TIME_STEP * (lame * lateral_vx + normal * depth_vz)
    next_xz = load_lines(xz_ref) + TIME_STEP * shear * (depth_vx + lateral_vz)
    next_zz = jnp.where(surface & jnp.broadcast_to(land, (32, NZ)), 0.0, next_zz)
    next_xz = jnp.where(surface, 0.0, next_xz)
    store_lines(vx_out, next_vx)
    store_lines(vz_out, next_vz)
    store_lines(xx_out, next_xx)
    store_lines(zz_out, next_zz)
    store_lines(xz_out, next_xz)

    each_other(lambda step: in_copy(step).wait_send())
    each_other(lambda step: home_copy(step).wait_send())


def body(
    velocity_x, velocity_z, stress_xx, stress_zz, stress_xz, material, land_mask,
    density, lame_lambda, shear_modulus, continuation_land, continuation_sea, continuation_bottom,
):
    across = spectral(NX)
    depth = spectral(NZ + CONT)
    across_high, across_low = two_parts(across[:, :256].T)
    inner_high, inner_low = two_parts(depth[:NZ, :NZ].T)
    bound = depth[:NZ, NZ:].T.astype(np.float32)

    flat = [
        a.reshape(32 * TILES, LANES)
        for a in (velocity_x, velocity_z, stress_xx, stress_zz, stress_xz, material)
    ]
    vmem = pl.BlockSpec(memory_space=pltpu.VMEM)
    smem = pl.BlockSpec(memory_space=pltpu.SMEM)
    hbm = pl.BlockSpec(memory_space=pltpu.HBM)
    lines = pltpu.VMEM((32 * TILES, LANES), jnp.float32)
    outs = pl.pallas_call(
        kernel,
        out_shape=[jax.ShapeDtypeStruct((32 * TILES, LANES), jnp.float32)] * 5,
        in_specs=[hbm] * 6 + [vmem] + [smem] * 3 + [vmem] * 4 + [hbm] * 4,
        out_specs=[vmem] * 5,
        scratch_shapes=[lines] * 5 + [
            pltpu.VMEM((32 * TILES, LANES), jnp.int32),
            pltpu.VMEM((NZ, NZ), jnp.bfloat16),
            pltpu.VMEM((NZ, NZ), jnp.bfloat16),
            pltpu.VMEM((256, NX), jnp.bfloat16),
            pltpu.VMEM((256, NX), jnp.bfloat16),
            pltpu.VMEM((2, NZ, LANES), jnp.float32),
            pltpu.VMEM((OWNERS, CHUNK, LANES), jnp.float32),
            pltpu.VMEM((OWNERS, CHUNK, LANES), jnp.float32),
            pltpu.VMEM((OWNERS, ROWS, LANES), jnp.float32),
            pltpu.VMEM((OWNERS, ROWS, LANES), jnp.float32),
            pltpu.SemaphoreType.DMA((10,)),
            pltpu.SemaphoreType.DMA((OWNERS,)),
            pltpu.SemaphoreType.DMA((OWNERS,)),
            pltpu.SemaphoreType.DMA((OWNERS,)),
            pltpu.SemaphoreType.DMA((OWNERS,)),
        ],
        compiler_params=pltpu.CompilerParams(collective_id=0, has_side_effects=True),
    )(
        *flat, land_mask.reshape(1, 32), density, lame_lambda, shear_modulus,
        continuation_land, continuation_sea, continuation_bottom, jnp.asarray(bound),
        jnp.asarray(inner_high), jnp.asarray(inner_low),
        jnp.asarray(across_high), jnp.asarray(across_low),
    )
    return tuple(a.reshape(32, 1, NZ) for a in outs)


def solution(mesh):
    split = P("gx", "gy", None)
    return jax.shard_map(
        body,
        mesh=mesh,
        in_specs=(split,) * 6 + (P("gx", "gy"),) + (P(),) * 6,
        out_specs=(split,) * 5,
        check_vma=False,
    )
```

```python
import functools

import jax
import jax.numpy as jnp
import numpy as np
from jax import lax
from jax.experimental import pallas as pl
from jax.experimental.pallas import tpu as pltpu
from jax.sharding import PartitionSpec as P

NX = 1024
NZ = 384
LAYERS = 16
WINDOW = 27
CONT = 26
RING_X = 4
RING_Z = 8
OWNERS = 32
ROWS = 12
CHUNK = 16
LANES = 128
TILES = 3
TIME_STEP = 0.2
VMEM_KIB = 63900


def spectral(length):
    indices = np.arange(length)
    distance = np.mod(indices[:, None] - indices[None, :] + length // 2, length) - length // 2
    parity = 1.0 - 2.0 * np.mod(distance, 2)
    tangent = np.tan(np.pi * np.where(distance == 0, 1, distance) / length)
    return np.where(distance == 0, 0.0, parity * (np.pi / length) / tangent)


def two_parts(matrix):
    high = matrix.astype(np.float32).astype(jnp.bfloat16)
    low = (matrix.astype(np.float32) - high.astype(np.float32)).astype(jnp.bfloat16)
    return high, low


def parts_of(value):
    high = value.astype(jnp.bfloat16)
    low = (value - high.astype(jnp.float32)).astype(jnp.bfloat16)
    return high, low


def dot(left, right):
    return jnp.dot(left, right, preferred_element_type=jnp.float32)


def split_product(left, right_high, right_low):
    rows = left.shape[0]
    high, low = parts_of(left)
    both = dot(jnp.concatenate([high, low], axis=0), right_high)
    return both[:rows] + (both[rows:] + dot(high, right_low))


def swap_blocks(arrays):
    lane = lax.broadcasted_iota(jnp.int32, arrays[0].shape, 1)
    out = list(arrays)
    for bit, width in ((1, 32), (2, 64)):
        upper = (lane & width) != 0
        for k in range(4):
            if k & bit:
                continue
            first, second = out[k], out[k | bit]
            out[k] = jnp.where(upper, pltpu.roll(second, width, 1), first)
            out[k | bit] = jnp.where(upper, second, pltpu.roll(first, LANES - width, 1))
    return out


def lateral(fields, across_high, across_low):
    pairs = []
    for field in fields:
        blocks = field.reshape(4, 2, CHUNK, LANES)
        pairs.append(
            jnp.concatenate(
                [blocks[:, 0].reshape(64, LANES), blocks[:, 1].reshape(64, LANES)], axis=1
            )
        )
    spread = split_product(jnp.concatenate(pairs, axis=0), across_high, across_low)
    results = []
    for f in range(len(fields)):
        pieces = []
        for target in range(4):
            total = None
            for source in range(4):
                shift = (target - source) % 4
                row = 64 * f + CHUNK * source
                term = spread[row : row + CHUNK, 256 * shift : 256 * shift + 256]
                total = term if total is None else total + term
            pieces += [total[:, :LANES], total[:, LANES:]]
        results.append(jnp.concatenate(pieces, axis=0))
    return results


def vertical(lines, land, inner_high, inner_low, edge_high, edge_low):
    lane = lax.broadcasted_iota(jnp.int32, (lines.shape[0], LANES), 1)
    upper = jnp.where(lane < WINDOW, lines[:, :LANES], 0.0)
    lower = jnp.where(lane >= LANES - WINDOW, lines[:, NZ - LANES :], 0.0)
    edges = (
        jnp.where(land, upper, 0.0)
        + pltpu.roll(jnp.where(land, 0.0, upper), 32, 1)
        + pltpu.roll(lower, 64 + WINDOW, 1)
    )
    return split_product(lines, inner_high, inner_low) + split_product(edges, edge_high, edge_low)


def load_lines(ref):
    return jnp.concatenate([ref[pl.ds(t, 32, stride=TILES), :] for t in range(TILES)], axis=1)


def store_lines(ref, value):
    for t in range(TILES):
        ref[pl.ds(t, 32, stride=TILES), :] = value[:, LANES * t : LANES * (t + 1)]


def kernel(
    vx_hbm, vz_hbm, xx_hbm, zz_hbm, xz_hbm, material_hbm,
    land_hbm, density_hbm, lame_hbm, shear_hbm, gland_hbm, gsea_hbm, gbottom_hbm, bound_hbm,
    inner_high_hbm, inner_low_hbm, across_high_hbm, across_low_hbm,
    home, coefs, side, edge_high_out, edge_low_out, inner_high_ref, inner_low_ref,
    xx_ref, zz_ref, xz_ref,
    vx_ref, vz_ref, material_ref, land_ref, density_ref, lame_ref, shear_ref,
    gland_ref, gsea_ref, gbottom_ref, bound_ref, across_high_ref, across_low_ref,
    packed, outgoing, incoming, returned, load_sem,
    send_sem, recv_sem, send_back_sem, recv_back_sem,
):
    me = lax.axis_index("gx")
    my_x, my_z = me // RING_Z, me % RING_Z

    def offset(step):
        group = step // 4
        half = (group + 1) // 2
        dz = 4 + half * (1 - 2 * (group % 2))
        dx = (2 + (step % 4)) % 4
        return dx, dz

    def ahead(step):
        dx, dz = offset(step)
        return ((my_x + dx) % RING_X) * RING_Z + (my_z + dz) % RING_Z

    def behind(step):
        dx, dz = offset(step)
        return ((my_x + RING_X - dx) % RING_X) * RING_Z + (my_z + 2 * RING_Z - dz) % RING_Z

    def is_other(step):
        dx, dz = offset(step)
        return dx + (dz % RING_Z) != 0

    barrier = pltpu.get_barrier_semaphore()

    def greet(step, carry):
        @pl.when(is_other(step))
        def _():
            pl.semaphore_signal(barrier, inc=1, device_id={"gx": ahead(step)})

        return carry

    lax.fori_loop(0, OWNERS, greet, 0)

    pairs = (
        (land_hbm, land_ref), (gland_hbm, gland_ref), (gsea_hbm, gsea_ref),
        (gbottom_hbm, gbottom_ref), (bound_hbm, bound_ref),
        (density_hbm, density_ref), (lame_hbm, lame_ref), (shear_hbm, shear_ref),
        (material_hbm, material_ref), (xz_hbm, xz_ref), (zz_hbm, zz_ref),
        (inner_high_hbm, inner_high_ref), (inner_low_hbm, inner_low_ref),
        (vx_hbm, vx_ref), (vz_hbm, vz_ref), (xx_hbm, xx_ref),
        (across_high_hbm, across_high_ref), (across_low_hbm, across_low_ref),
    )
    loads = [pltpu.make_async_copy(a, b, load_sem.at[i]) for i, (a, b) in enumerate(pairs)]
    for load in loads:
        load.start()
    for load in loads[:5]:
        load.wait()

    diagonal = lax.broadcasted_iota(jnp.int32, (32, 32), 0) == lax.broadcasted_iota(
        jnp.int32, (32, 32), 1
    )
    land = (
        jnp.sum(
            jnp.where(diagonal, jnp.broadcast_to(land_ref[...], (32, 32)), 0),
            axis=1,
            keepdims=True,
        )
        > 0
    )
    land_pair = jnp.broadcast_to(jnp.concatenate([land, land], axis=0), (64, LANES))
    side[...] = land_pair.astype(jnp.int32)

    gap = jnp.zeros((CONT, 32 - WINDOW), jnp.float32)
    grams = jnp.concatenate(
        [gland_ref[...], gap, gsea_ref[...], gap, gbottom_ref[...], gap,
         jnp.zeros((CONT, 32), jnp.float32)],
        axis=1,
    )
    folded = lax.dot_general(
        grams, bound_ref[...], (((0,), (0,)), ((), ())),
        precision=lax.Precision.HIGHEST, preferred_element_type=jnp.float32,
    )
    edge_high, edge_low = parts_of(folded)
    edge_high_out[...] = edge_high
    edge_low_out[...] = edge_low

    for load in loads[5:9]:
        load.wait()
    material = load_lines(material_ref)
    density = jnp.full(material.shape, density_ref[0], jnp.float32)
    lame = jnp.full(material.shape, lame_ref[0], jnp.float32)
    shear = jnp.full(material.shape, shear_ref[0], jnp.float32)
    for layer in range(1, LAYERS):
        chosen = material == layer
        density = jnp.where(chosen, density_ref[layer], density)
        lame = jnp.where(chosen, lame_ref[layer], lame)
        shear = jnp.where(chosen, shear_ref[layer], shear)
    light = TIME_STEP * (1.0 / density)
    coefs[0] = lame
    coefs[1] = shear

    for load in loads[9:13]:
        load.wait()
    inner_high, inner_low = inner_high_ref[...], inner_low_ref[...]
    stress_xz = load_lines(xz_ref)
    stress_zz = load_lines(zz_ref)
    depth = vertical(
        jnp.concatenate([stress_xz, stress_zz], axis=0), land_pair,
        inner_high, inner_low, edge_high, edge_low,
    )
    for load in loads[13:16]:
        load.wait()
    stress_xx = load_lines(xx_ref)
    part_vx = load_lines(vx_ref) + light * depth[:32]
    part_vz = load_lines(vz_ref) + light * depth[32:]

    packed[0] = jnp.concatenate([stress_xx, stress_xz, part_vx, part_vz], axis=0).T
    packed[1] = jnp.concatenate(
        [light] + [pltpu.roll(light, NZ - 3 * slot, 1) for slot in range(1, 4)], axis=0
    ).T
    for owner in range(OWNERS):
        outgoing[owner, :ROWS] = packed[0, ROWS * owner : ROWS * (owner + 1)]
        outgoing[owner, ROWS:] = packed[1, ROWS * owner : ROWS * owner + CHUNK - ROWS]
    incoming[me] = outgoing[me]

    pl.semaphore_wait(barrier, OWNERS - 1)

    def out_copy(step):
        return pltpu.make_async_remote_copy(
            src_ref=outgoing.at[ahead(step)], dst_ref=incoming.at[me],
            send_sem=send_sem.at[step], recv_sem=recv_sem.at[step],
            device_id={"gx": ahead(step)},
        )

    def in_copy(step):
        return pltpu.make_async_remote_copy(
            src_ref=outgoing.at[ahead(step)], dst_ref=incoming.at[behind(step)],
            send_sem=send_sem.at[step], recv_sem=recv_sem.at[step],
            device_id={"gx": ahead(step)},
        )

    def back_copy(step):
        return pltpu.make_async_remote_copy(
            src_ref=returned.at[ahead(step)], dst_ref=home.at[me],
            send_sem=send_back_sem.at[step], recv_sem=recv_back_sem.at[step],
            device_id={"gx": ahead(step)},
        )

    def home_copy(step):
        return pltpu.make_async_remote_copy(
            src_ref=returned.at[ahead(step)], dst_ref=home.at[behind(step)],
            send_sem=send_back_sem.at[step], recv_sem=recv_back_sem.at[step],
            device_id={"gx": ahead(step)},
        )

    def each_other(act):
        def step_of(step, carry):
            @pl.when(is_other(step))
            def _():
                act(step)

            return carry

        lax.fori_loop(0, OWNERS, step_of, 0)

    each_other(lambda step: out_copy(step).start())
    each_other(lambda step: in_copy(step).wait_recv())
    for load in loads[16:]:
        load.wait()
    across_high, across_low = across_high_ref[...], across_low_ref[...]

    got = incoming[...].reshape(8, 4, CHUNK, LANES)
    fields = swap_blocks([got[:, k].reshape(8 * CHUNK, LANES) for k in range(4)])
    row = lax.broadcasted_iota(jnp.int32, (8 * CHUNK, LANES), 0) % CHUNK
    factor = jnp.zeros((8 * CHUNK, LANES), jnp.float32)
    for slot in range(4):
        moved = pltpu.roll(fields[slot], 8 * CHUNK + 3 * slot - ROWS, 0)
        factor = jnp.where((row >= 3 * slot) & (row < 3 * slot + 3), moved, factor)
    slope = lateral(fields[:2], across_high, across_low)
    moved_vx = fields[2] + factor * slope[0]
    moved_vz = fields[3] + factor * slope[1]
    slope = lateral([moved_vx, moved_vz], across_high, across_low)
    back = swap_blocks([moved_vx, moved_vz, slope[0], slope[1]])
    for k in range(4):
        for group in range(8):
            returned[4 * group + k] = back[k][CHUNK * group : CHUNK * group + ROWS]
    home[me] = returned[me]

    each_other(lambda step: back_copy(step).start())
    each_other(lambda step: home_copy(step).wait_recv())

    each_other(lambda step: in_copy(step).wait_send())
    each_other(lambda step: home_copy(step).wait_send())


def last_kernel(
    home, coefs, side, edge_high_ref, edge_low_ref, inner_high_ref, inner_low_ref,
    xx_ref, zz_ref, xz_ref,
    vx_out, vz_out, xx_out, zz_out, xz_out,
    packed,
):
    for owner in range(OWNERS):
        packed[ROWS * owner : ROWS * (owner + 1)] = home[owner]
    settled = packed[...].T
    next_vx, next_vz = settled[:32], settled[32:64]
    store_lines(vx_out, next_vx)
    store_lines(vz_out, next_vz)
    lateral_vx, lateral_vz = settled[64:96], settled[96:]
    land = side[...] > 0
    depth = vertical(
        settled[:64], land, inner_high_ref[...], inner_low_ref[...],
        edge_high_ref[...], edge_low_ref[...],
    )
    depth_vx, depth_vz = depth[:32], depth[32:]
    lame, shear = coefs[0], coefs[1]
    normal = lame + 2.0 * shear
    surface = lax.broadcasted_iota(jnp.int32, (32, NZ), 1) == 0
    next_xx = load_lines(xx_ref) + TIME_STEP * (normal * lateral_vx + lame * depth_vz)
    next_zz = load_lines(zz_ref) + TIME_STEP * (lame * lateral_vx + normal * depth_vz)
    next_xz = load_lines(xz_ref) + TIME_STEP * shear * (depth_vx + lateral_vz)
    on_land = jnp.concatenate([land[:32]] * TILES, axis=1)
    next_zz = jnp.where(surface & on_land, 0.0, next_zz)
    next_xz = jnp.where(surface, 0.0, next_xz)
    store_lines(xx_out, next_xx)
    store_lines(zz_out, next_zz)
    store_lines(xz_out, next_xz)


def body(
    velocity_x, velocity_z, stress_xx, stress_zz, stress_xz, material, land_mask,
    density, lame_lambda, shear_modulus, continuation_land, continuation_sea, continuation_bottom,
):
    across = spectral(NX)
    depth = spectral(NZ + CONT)
    across_high, across_low = two_parts(across[:, :256].T)
    inner_high, inner_low = two_parts(depth[:NZ, :NZ].T)
    bound = depth[:NZ, NZ:].T.astype(np.float32)

    flat = [
        a.reshape(32 * TILES, LANES)
        for a in (velocity_x, velocity_z, stress_xx, stress_zz, stress_xz, material)
    ]
    vmem = pl.BlockSpec(memory_space=pltpu.VMEM)
    hbm = pl.BlockSpec(memory_space=pltpu.HBM)
    lines = pltpu.VMEM((32 * TILES, LANES), jnp.float32)
    square = pltpu.VMEM((NZ, NZ), jnp.bfloat16)
    edge = pltpu.VMEM((LANES, NZ), jnp.bfloat16)
    gram = pltpu.VMEM((CONT, WINDOW), jnp.float32)
    layers = pltpu.SMEM((LAYERS,), jnp.float32)
    kept = pl.pallas_call(
        kernel,
        out_shape=[
            pltpu.VMEM((OWNERS, ROWS, LANES), jnp.float32),
            pltpu.VMEM((2, 32, NZ), jnp.float32),
            pltpu.VMEM((64, LANES), jnp.int32),
            edge, edge, square, square, lines, lines, lines,
        ],
        in_specs=[hbm] * 18,
        out_specs=[vmem] * 10,
        scratch_shapes=[
            lines, lines,
            pltpu.VMEM((32 * TILES, LANES), jnp.int32),
            pltpu.VMEM((1, 32), jnp.int32),
            layers, layers, layers, gram, gram, gram,
            pltpu.VMEM((CONT, NZ), jnp.float32),
            pltpu.VMEM((256, NX), jnp.bfloat16),
            pltpu.VMEM((256, NX), jnp.bfloat16),
            pltpu.VMEM((2, NZ, LANES), jnp.float32),
            pltpu.VMEM((OWNERS, CHUNK, LANES), jnp.float32),
            pltpu.VMEM((OWNERS, CHUNK, LANES), jnp.float32),
            pltpu.VMEM((OWNERS, ROWS, LANES), jnp.float32),
            pltpu.SemaphoreType.DMA((18,)),
            pltpu.SemaphoreType.DMA((OWNERS,)),
            pltpu.SemaphoreType.DMA((OWNERS,)),
            pltpu.SemaphoreType.DMA((OWNERS,)),
            pltpu.SemaphoreType.DMA((OWNERS,)),
        ],
        compiler_params=pltpu.CompilerParams(
            collective_id=0, has_side_effects=True, vmem_limit_bytes=VMEM_KIB * 1024
        ),
    )(
        *flat, land_mask.reshape(1, 32), density, lame_lambda, shear_modulus,
        continuation_land, continuation_sea, continuation_bottom, jnp.asarray(bound),
        jnp.asarray(inner_high), jnp.asarray(inner_low),
        jnp.asarray(across_high), jnp.asarray(across_low),
    )
    outs = pl.pallas_call(
        last_kernel,
        out_shape=[jax.ShapeDtypeStruct((32 * TILES, LANES), jnp.float32)] * 5,
        in_specs=[vmem] * 10,
        out_specs=[vmem] * 5,
        scratch_shapes=[pltpu.VMEM((NZ, LANES), jnp.float32)],
        compiler_params=pltpu.CompilerParams(vmem_limit_bytes=8 * 2**20),
    )(*kept)
    return tuple(a.reshape(32, 1, NZ) for a in outs)


def solution(mesh):
    split = P("gx", "gy", None)
    return jax.shard_map(
        body,
        mesh=mesh,
        in_specs=(split,) * 6 + (P("gx", "gy"),) + (P(),) * 6,
        out_specs=(split,) * 5,
        check_vma=False,
    )
```

```python
import functools

import jax
import jax.numpy as jnp
import numpy as np
from jax import lax
from jax.experimental import pallas as pl
from jax.experimental.pallas import tpu as pltpu
from jax.sharding import PartitionSpec as P

NX = 1024
NZ = 384
LAYERS = 16
WINDOW = 27
CONT = 26
RING_X = 4
RING_Z = 8
OWNERS = 32
ROWS = 12
CHUNK = 16
LANES = 128
TILES = 3
TIME_STEP = 0.2
VMEM_KIB = 63900


ORDER = [
    (dx, sign * dz % RING_Z)
    for dz in (4, 3, 2, 1, 0)
    for dx in (2, 1, 3, 0)
    for sign in ((1, -1) if dz % 4 else (1,))
    if dx or dz
]
PIECES = (4, 8)


def spectral(length):
    indices = np.arange(length)
    distance = np.mod(indices[:, None] - indices[None, :] + length // 2, length) - length // 2
    parity = 1.0 - 2.0 * np.mod(distance, 2)
    tangent = np.tan(np.pi * np.where(distance == 0, 1, distance) / length)
    return np.where(distance == 0, 0.0, parity * (np.pi / length) / tangent)


def two_parts(matrix):
    high = matrix.astype(np.float32).astype(jnp.bfloat16)
    low = (matrix.astype(np.float32) - high.astype(np.float32)).astype(jnp.bfloat16)
    return high, low


def parts_of(value):
    high = value.astype(jnp.bfloat16)
    low = (value - high.astype(jnp.float32)).astype(jnp.bfloat16)
    return high, low


def dot(left, right):
    return jnp.dot(left, right, preferred_element_type=jnp.float32)


def split_product(left, right_high, right_low):
    rows = left.shape[0]
    high, low = parts_of(left)
    both = dot(jnp.concatenate([high, low], axis=0), right_high)
    return both[:rows] + (both[rows:] + dot(high, right_low))


def swap_blocks(arrays):
    lane = lax.broadcasted_iota(jnp.int32, arrays[0].shape, 1)
    out = list(arrays)
    for bit, width in ((1, 32), (2, 64)):
        upper = (lane & width) != 0
        for k in range(4):
            if k & bit:
                continue
            first, second = out[k], out[k | bit]
            out[k] = jnp.where(upper, pltpu.roll(second, width, 1), first)
            out[k | bit] = jnp.where(upper, second, pltpu.roll(first, LANES - width, 1))
    return out


def lateral(fields, across_high, across_low):
    height = fields[0].shape[0] // 8
    pairs = []
    for field in fields:
        blocks = field.reshape(4, 2, height, LANES)
        pairs.append(
            jnp.concatenate(
                [blocks[:, half].reshape(4 * height, LANES) for half in range(2)], axis=1
            )
        )
    spread = split_product(jnp.concatenate(pairs, axis=0), across_high, across_low)
    results = []
    for f in range(len(fields)):
        pieces = []
        for target in range(4):
            total = None
            for source in range(4):
                shift = (target - source) % 4
                row = height * (4 * f + source)
                term = spread[row : row + height, 256 * shift : 256 * shift + 256]
                total = term if total is None else total + term
            pieces += [total[:, :LANES], total[:, LANES:]]
        results.append(jnp.concatenate(pieces, axis=0))
    return results


def vertical(lines, land, inner_high, inner_low, edge_high, edge_low):
    lane = lax.broadcasted_iota(jnp.int32, (lines.shape[0], LANES), 1)
    upper = jnp.where(lane < WINDOW, lines[:, :LANES], 0.0)
    lower = jnp.where(lane >= LANES - WINDOW, lines[:, NZ - LANES :], 0.0)
    edges = (
        jnp.where(land, upper, 0.0)
        + pltpu.roll(jnp.where(land, 0.0, upper), 32, 1)
        + pltpu.roll(lower, 64 + WINDOW, 1)
    )
    return split_product(lines, inner_high, inner_low) + split_product(edges, edge_high, edge_low)


def load_lines(ref):
    return jnp.concatenate([ref[pl.ds(t, 32, stride=TILES), :] for t in range(TILES)], axis=1)


def store_lines(ref, value):
    for t in range(TILES):
        ref[pl.ds(t, 32, stride=TILES), :] = value[:, LANES * t : LANES * (t + 1)]


def kernel(
    vx_hbm, vz_hbm, xx_hbm, zz_hbm, xz_hbm, material_hbm,
    land_hbm, density_hbm, lame_hbm, shear_hbm, gland_hbm, gsea_hbm, gbottom_hbm, bound_hbm,
    inner_high_hbm, inner_low_hbm, across_high_hbm, across_low_hbm,
    *refs,
):
    n = len(PIECES)
    home, refs = refs[:n], refs[n:]
    (
    coefs, side, edge_high_out, edge_low_out, inner_high_ref, inner_low_ref,
    xx_ref, zz_ref, xz_ref,
    vx_ref, vz_ref, material_ref, land_ref, density_ref, lame_ref, shear_ref,
    gland_ref, gsea_ref, gbottom_ref, bound_ref, across_high_ref, across_low_ref,
    packed,
    ) = refs[:-5 - 3 * n]
    outgoing, incoming, returned = refs[-5 - 3 * n:-5 - 2 * n], refs[-5 - 2 * n:-5 - n], refs[-5 - n:-5]
    load_sem, send_sem, recv_sem, send_back_sem, recv_back_sem = refs[-5:]
    me = lax.axis_index("gx")
    my_x, my_z = lax.div(me, RING_Z), lax.rem(me, RING_Z)
    along_x = [lax.rem(my_x + dx, RING_X) * RING_Z for dx in range(RING_X)]
    along_z = [lax.rem(my_z + dz, RING_Z) for dz in range(RING_Z)]
    others = [along_x[dx] + along_z[dz] for dx, dz in ORDER]

    barrier = pltpu.get_barrier_semaphore()
    for other in others:
        pl.semaphore_signal(barrier, inc=1, device_id={"gx": other})

    pairs = (
        (land_hbm, land_ref), (gland_hbm, gland_ref), (gsea_hbm, gsea_ref),
        (gbottom_hbm, gbottom_ref), (bound_hbm, bound_ref),
        (density_hbm, density_ref), (lame_hbm, lame_ref), (shear_hbm, shear_ref),
        (material_hbm, material_ref), (xz_hbm, xz_ref), (zz_hbm, zz_ref),
        (inner_high_hbm, inner_high_ref), (inner_low_hbm, inner_low_ref),
        (vx_hbm, vx_ref), (vz_hbm, vz_ref), (xx_hbm, xx_ref),
        (across_high_hbm, across_high_ref), (across_low_hbm, across_low_ref),
    )
    loads = [pltpu.make_async_copy(a, b, load_sem.at[i]) for i, (a, b) in enumerate(pairs)]
    for load in loads:
        load.start()
    for load in loads[:5]:
        load.wait()

    diagonal = lax.broadcasted_iota(jnp.int32, (32, 32), 0) == lax.broadcasted_iota(
        jnp.int32, (32, 32), 1
    )
    land = (
        jnp.sum(
            jnp.where(diagonal, jnp.broadcast_to(land_ref[...], (32, 32)), 0),
            axis=1,
            keepdims=True,
        )
        > 0
    )
    land_pair = jnp.broadcast_to(jnp.concatenate([land, land], axis=0), (64, LANES))
    side[...] = land_pair.astype(jnp.int32)

    gap = jnp.zeros((CONT, 32 - WINDOW), jnp.float32)
    grams = jnp.concatenate(
        [gland_ref[...], gap, gsea_ref[...], gap, gbottom_ref[...], gap,
         jnp.zeros((CONT, 32), jnp.float32)],
        axis=1,
    )
    folded = lax.dot_general(
        grams, bound_ref[...], (((0,), (0,)), ((), ())),
        precision=lax.Precision.HIGHEST, preferred_element_type=jnp.float32,
    )
    edge_high, edge_low = parts_of(folded)
    edge_high_out[...] = edge_high
    edge_low_out[...] = edge_low

    for load in loads[5:9]:
        load.wait()
    material = load_lines(material_ref)
    density = jnp.full(material.shape, density_ref[0], jnp.float32)
    lame = jnp.full(material.shape, lame_ref[0], jnp.float32)
    shear = jnp.full(material.shape, shear_ref[0], jnp.float32)
    for layer in range(1, LAYERS):
        chosen = material == layer
        density = jnp.where(chosen, density_ref[layer], density)
        lame = jnp.where(chosen, lame_ref[layer], lame)
        shear = jnp.where(chosen, shear_ref[layer], shear)
    light = TIME_STEP * (1.0 / density)
    coefs[0] = lame
    coefs[1] = shear

    for load in loads[9:13]:
        load.wait()
    inner_high, inner_low = inner_high_ref[...], inner_low_ref[...]
    stress_xz = load_lines(xz_ref)
    stress_zz = load_lines(zz_ref)
    depth = vertical(
        jnp.concatenate([stress_xz, stress_zz], axis=0), land_pair,
        inner_high, inner_low, edge_high, edge_low,
    )
    for load in loads[13:16]:
        load.wait()
    stress_xx = load_lines(xx_ref)
    part_vx = load_lines(vx_ref) + light * depth[:32]
    part_vz = load_lines(vz_ref) + light * depth[32:]

    packed[0] = jnp.concatenate([stress_xx, stress_xz, part_vx, part_vz], axis=0).T
    packed[1] = jnp.concatenate(
        [light] + [pltpu.roll(light, NZ - slot, 1) for slot in range(1, 4)], axis=0
    ).T
    first = 0
    for piece, rows in enumerate(PIECES):
        for owner in range(OWNERS):
            start = ROWS * owner + first
            outgoing[piece][owner, :rows] = packed[0, start : start + rows]
            for i in range(rows // 4):
                outgoing[piece][owner, rows + i : rows + i + 1] = packed[
                    1, start + 4 * i : start + 4 * i + 1
                ]
        incoming[piece][me, : rows + rows // 4] = outgoing[piece][me]
        first += rows

    pl.semaphore_wait(barrier, OWNERS - 1)

    def send(source, target, send_semaphore, recv_semaphore):
        for other in others:
            pltpu.make_async_remote_copy(
                src_ref=source.at[other], dst_ref=target.at[me],
                send_sem=send_semaphore, recv_sem=recv_semaphore, device_id={"gx": other},
            ).start()

    def all_of(source, target, send_semaphore, recv_semaphore):
        return pltpu.make_async_remote_copy(
            src_ref=source.at[pl.ds(0, OWNERS - 1)], dst_ref=target.at[pl.ds(0, OWNERS - 1)],
            send_sem=send_semaphore, recv_sem=recv_semaphore, device_id={"gx": others[0]},
        )

    there, back = [], []
    for piece, rows in enumerate(PIECES):
        landing = incoming[piece].at[:, pl.ds(0, rows + rows // 4)]
        there.append((outgoing[piece], landing, send_sem.at[piece], recv_sem.at[piece]))
        back.append((returned[piece], home[piece], send_back_sem.at[piece], recv_back_sem.at[piece]))
        send(*there[piece])
    for load in loads[16:]:
        load.wait()
    across_high, across_low = across_high_ref[...], across_low_ref[...]

    for piece, rows in enumerate(PIECES):
        all_of(*there[piece]).wait_recv()
        height = 2 * rows
        got = incoming[piece][...].reshape(8, 4, height, LANES)
        fields = swap_blocks([got[:, k].reshape(8 * height, LANES) for k in range(4)])
        row = lax.broadcasted_iota(jnp.int32, (8 * height, LANES), 0) % height
        factor = jnp.zeros((8 * height, LANES), jnp.float32)
        for i in range(rows // 4):
            for slot in range(4):
                target = 4 * i + slot
                moved = pltpu.roll(fields[slot], 8 * height + target - (rows + i), 0)
                factor = jnp.where(row == target, moved, factor)
        slope = lateral(fields[:2], across_high, across_low)
        moved_vx = fields[2] + factor * slope[0]
        moved_vz = fields[3] + factor * slope[1]
        slope = lateral([moved_vx, moved_vz], across_high, across_low)
        result = swap_blocks([moved_vx, moved_vz, slope[0], slope[1]])
        for k in range(4):
            for group in range(8):
                returned[piece][4 * group + k] = result[k][height * group : height * group + rows]
        home[piece][me] = returned[piece][me]
        send(*back[piece])

    for piece in range(len(PIECES)):
        all_of(*back[piece]).wait_recv()
    for piece in range(len(PIECES)):
        all_of(*there[piece]).wait_send()
        all_of(*back[piece]).wait_send()


def last_kernel(*refs):
    n = len(PIECES)
    home, refs = refs[:n], refs[n:]
    (
    coefs, side, edge_high_ref, edge_low_ref, inner_high_ref, inner_low_ref,
    xx_ref, zz_ref, xz_ref,
    vx_out, vz_out, xx_out, zz_out, xz_out,
    packed,
    ) = refs
    first = 0
    for piece, rows in enumerate(PIECES):
        for owner in range(OWNERS):
            start = ROWS * owner + first
            packed[start : start + rows] = home[piece][owner]
        first += rows
    settled = packed[...].T
    next_vx, next_vz = settled[:32], settled[32:64]
    store_lines(vx_out, next_vx)
    store_lines(vz_out, next_vz)
    lateral_vx, lateral_vz = settled[64:96], settled[96:]
    land = side[...] > 0
    depth = vertical(
        settled[:64], land, inner_high_ref[...], inner_low_ref[...],
        edge_high_ref[...], edge_low_ref[...],
    )
    depth_vx, depth_vz = depth[:32], depth[32:]
    lame, shear = coefs[0], coefs[1]
    normal = lame + 2.0 * shear
    surface = lax.broadcasted_iota(jnp.int32, (32, NZ), 1) == 0
    next_xx = load_lines(xx_ref) + TIME_STEP * (normal * lateral_vx + lame * depth_vz)
    next_zz = load_lines(zz_ref) + TIME_STEP * (lame * lateral_vx + normal * depth_vz)
    next_xz = load_lines(xz_ref) + TIME_STEP * shear * (depth_vx + lateral_vz)
    on_land = jnp.concatenate([land[:32]] * TILES, axis=1)
    next_zz = jnp.where(surface & on_land, 0.0, next_zz)
    next_xz = jnp.where(surface, 0.0, next_xz)
    store_lines(xx_out, next_xx)
    store_lines(zz_out, next_zz)
    store_lines(xz_out, next_xz)


def body(
    velocity_x, velocity_z, stress_xx, stress_zz, stress_xz, material, land_mask,
    density, lame_lambda, shear_modulus, continuation_land, continuation_sea, continuation_bottom,
):
    across = spectral(NX)
    depth = spectral(NZ + CONT)
    across_high, across_low = two_parts(across[:, :256].T)
    inner_high, inner_low = two_parts(depth[:NZ, :NZ].T)
    bound = depth[:NZ, NZ:].T.astype(np.float32)

    flat = [
        a.reshape(32 * TILES, LANES)
        for a in (velocity_x, velocity_z, stress_xx, stress_zz, stress_xz, material)
    ]
    vmem = pl.BlockSpec(memory_space=pltpu.VMEM)
    hbm = pl.BlockSpec(memory_space=pltpu.HBM)
    lines = pltpu.VMEM((32 * TILES, LANES), jnp.float32)
    square = pltpu.VMEM((NZ, NZ), jnp.bfloat16)
    edge = pltpu.VMEM((LANES, NZ), jnp.bfloat16)
    gram = pltpu.VMEM((CONT, WINDOW), jnp.float32)
    layers = pltpu.SMEM((LAYERS,), jnp.float32)
    kept = pl.pallas_call(
        kernel,
        out_shape=[
            *[pltpu.VMEM((OWNERS, rows, LANES), jnp.float32) for rows in PIECES],
            pltpu.VMEM((2, 32, NZ), jnp.float32),
            pltpu.VMEM((64, LANES), jnp.int32),
            edge, edge, square, square, lines, lines, lines,
        ],
        in_specs=[hbm] * 18,
        out_specs=[vmem] * (9 + len(PIECES)),
        scratch_shapes=[
            lines, lines,
            pltpu.VMEM((32 * TILES, LANES), jnp.int32),
            pltpu.VMEM((1, 32), jnp.int32),
            layers, layers, layers, gram, gram, gram,
            pltpu.VMEM((CONT, NZ), jnp.float32),
            pltpu.VMEM((256, NX), jnp.bfloat16),
            pltpu.VMEM((256, NX), jnp.bfloat16),
            pltpu.VMEM((2, NZ, LANES), jnp.float32),
            *[pltpu.VMEM((OWNERS, rows + rows // 4, LANES), jnp.float32) for rows in PIECES],
            *[pltpu.VMEM((OWNERS, 2 * rows, LANES), jnp.float32) for rows in PIECES],
            *[pltpu.VMEM((OWNERS, rows, LANES), jnp.float32) for rows in PIECES],
            pltpu.SemaphoreType.DMA((18,)),
            *[pltpu.SemaphoreType.DMA((len(PIECES),))] * 4,
        ],
        compiler_params=pltpu.CompilerParams(
            collective_id=0, has_side_effects=True, vmem_limit_bytes=VMEM_KIB * 1024
        ),
    )(
        *flat, land_mask.reshape(1, 32), density, lame_lambda, shear_modulus,
        continuation_land, continuation_sea, continuation_bottom, jnp.asarray(bound),
        jnp.asarray(inner_high), jnp.asarray(inner_low),
        jnp.asarray(across_high), jnp.asarray(across_low),
    )
    outs = pl.pallas_call(
        last_kernel,
        out_shape=[jax.ShapeDtypeStruct((32 * TILES, LANES), jnp.float32)] * 5,
        in_specs=[vmem] * (9 + len(PIECES)),
        out_specs=[vmem] * 5,
        scratch_shapes=[pltpu.VMEM((NZ, LANES), jnp.float32)],
        compiler_params=pltpu.CompilerParams(vmem_limit_bytes=8 * 2**20),
    )(*kept)
    return tuple(a.reshape(32, 1, NZ) for a in outs)


def solution(mesh):
    split = P("gx", "gy", None)
    return jax.shard_map(
        body,
        mesh=mesh,
        in_specs=(split,) * 6 + (P("gx", "gy"),) + (P(),) * 6,
        out_specs=(split,) * 5,
        check_vma=False,
    )
```

```python
import functools

import jax
import jax.numpy as jnp
import numpy as np
from jax import lax
from jax.experimental import pallas as pl
from jax.experimental.pallas import tpu as pltpu
from jax.sharding import PartitionSpec as P

NX = 1024
NZ = 384
LAYERS = 16
WINDOW = 27
CONT = 26
RING_X = 4
RING_Z = 8
OWNERS = 32
HALF = RING_Z // 2
LATE_X = 2
HOLDERS = RING_X * HALF + LATE_X * HALF
ROWS = NZ // HOLDERS
LANES = 128
TILES = 3
TIME_STEP = 0.2
VMEM_KIB = 63900
PIECES = (4, 4, 8)


def chunk_rows(rows):
    return rows + rows // 4


def height_of(rows):
    return -(-chunk_rows(rows) // 8) * 8


def block_of(rows):
    return max(rows, 8)


def spectral(length):
    indices = np.arange(length)
    distance = np.mod(indices[:, None] - indices[None, :] + length // 2, length) - length // 2
    parity = 1.0 - 2.0 * np.mod(distance, 2)
    tangent = np.tan(np.pi * np.where(distance == 0, 1, distance) / length)
    return np.where(distance == 0, 0.0, parity * (np.pi / length) / tangent)


def two_parts(matrix):
    high = matrix.astype(np.float32).astype(jnp.bfloat16)
    low = (matrix.astype(np.float32) - high.astype(np.float32)).astype(jnp.bfloat16)
    return high, low


def parts_of(value):
    high = value.astype(jnp.bfloat16)
    low = (value - high.astype(jnp.float32)).astype(jnp.bfloat16)
    return high, low


def dot(left, right):
    return jnp.dot(left, right, preferred_element_type=jnp.float32)


def split_product(left, right_high, right_low):
    rows = left.shape[0]
    high, low = parts_of(left)
    both = dot(jnp.concatenate([high, low], axis=0), right_high)
    return both[:rows] + (both[rows:] + dot(high, right_low))


def swap_blocks(arrays):
    lane = lax.broadcasted_iota(jnp.int32, arrays[0].shape, 1)
    out = list(arrays)
    for bit, width in ((1, 32), (2, 64)):
        upper = (lane & width) != 0
        for k in range(4):
            if k & bit:
                continue
            first, second = out[k], out[k | bit]
            out[k] = jnp.where(upper, pltpu.roll(second, width, 1), first)
            out[k | bit] = jnp.where(upper, second, pltpu.roll(first, LANES - width, 1))
    return out


def lateral(fields, across_high, across_low):
    height = fields[0].shape[0] // 8
    pairs = []
    for field in fields:
        blocks = field.reshape(4, 2, height, LANES)
        pairs.append(
            jnp.concatenate(
                [blocks[:, half].reshape(4 * height, LANES) for half in range(2)], axis=1
            )
        )
    spread = split_product(jnp.concatenate(pairs, axis=0), across_high, across_low)
    results = []
    for f in range(len(fields)):
        pieces = []
        for target in range(4):
            total = None
            for source in range(4):
                shift = (target - source) % 4
                row = height * (4 * f + source)
                term = spread[row : row + height, 256 * shift : 256 * shift + 256]
                total = term if total is None else total + term
            pieces += [total[:, :LANES], total[:, LANES:]]
        results.append(jnp.concatenate(pieces, axis=0))
    return results


def vertical(lines, land, inner_high, inner_low, edge_high, edge_low):
    lane = lax.broadcasted_iota(jnp.int32, (lines.shape[0], LANES), 1)
    upper = jnp.where(lane < WINDOW, lines[:, :LANES], 0.0)
    lower = jnp.where(lane >= LANES - WINDOW, lines[:, NZ - LANES :], 0.0)
    edges = (
        jnp.where(land, upper, 0.0)
        + pltpu.roll(jnp.where(land, 0.0, upper), 32, 1)
        + pltpu.roll(lower, 64 + WINDOW, 1)
    )
    return split_product(lines, inner_high, inner_low) + split_product(edges, edge_high, edge_low)


def load_lines(ref):
    return jnp.concatenate([ref[pl.ds(t, 32, stride=TILES), :] for t in range(TILES)], axis=1)


def store_lines(ref, value):
    for t in range(TILES):
        ref[pl.ds(t, 32, stride=TILES), :] = value[:, LANES * t : LANES * (t + 1)]


def kernel(
    vx_hbm, vz_hbm, xx_hbm, zz_hbm, xz_hbm, material_hbm,
    land_hbm, density_hbm, lame_hbm, shear_hbm, gland_hbm, gsea_hbm, gbottom_hbm, bound_hbm,
    inner_high_hbm, inner_low_hbm, across_high_hbm, across_low_hbm,
    *refs,
):
    n = len(PIECES)
    home, refs = refs[:n], refs[n:]
    (
    coefs, side, edge_high_out, edge_low_out, inner_high_ref, inner_low_ref,
    xx_ref, zz_ref, xz_ref,
    vx_ref, vz_ref, material_ref, land_ref, density_ref, lame_ref, shear_ref,
    gland_ref, gsea_ref, gbottom_ref, bound_ref, across_high_ref, across_low_ref,
    packed,
    ) = refs[:-5 - 3 * n]
    outgoing, incoming, returned = refs[-5 - 3 * n:-5 - 2 * n], refs[-5 - 2 * n:-5 - n], refs[-5 - n:-5]
    load_sem, send_sem, recv_sem, send_back_sem, recv_back_sem = refs[-5:]
    me = lax.axis_index("gx")
    my_x, my_z = lax.div(me, RING_Z), lax.rem(me, RING_Z)
    early = my_z < HALF
    holding = early | (my_x < LATE_X)
    my_slot = jnp.where(early, my_x * HALF + my_z, RING_X * HALF + my_x * HALF + my_z - HALF)
    any_x = [lax.rem(my_x + dx, RING_X) for dx in range(RING_X)]
    late_x = [lax.rem(my_x + dx, LATE_X) for dx in range(LATE_X)]
    half_z = [lax.rem(my_z + dz, HALF) for dz in range(HALF)]

    def group(columns, first_z, first_slot, far):
        found = []
        for x in columns[::-1] if far else columns:
            for z in half_z[::-1] if far else half_z:
                found.append((x * RING_Z + first_z + z, first_slot + x * HALF + z))
        return found

    early_ones = group(any_x, 0, 0, True)
    late_holders = group(late_x, HALF, RING_X * HALF, True)
    late_ones = group(any_x, HALF, 0, True)

    def each_other(members, act):
        for index, (device, slot) in enumerate(members):
            if index < len(members) - 1:
                act(device, slot)
            else:
                pl.when(device != me)(functools.partial(act, device, slot))

    barrier = pltpu.get_barrier_semaphore()

    def greet(device, slot):
        pl.semaphore_signal(barrier, inc=1, device_id={"gx": device})

    @pl.when(holding)
    def _():
        each_other(early_ones, greet)
        each_other(late_ones, greet)

    pairs = (
        (land_hbm, land_ref), (gland_hbm, gland_ref), (gsea_hbm, gsea_ref),
        (gbottom_hbm, gbottom_ref), (bound_hbm, bound_ref),
        (density_hbm, density_ref), (lame_hbm, lame_ref), (shear_hbm, shear_ref),
        (material_hbm, material_ref), (xz_hbm, xz_ref), (zz_hbm, zz_ref),
        (inner_high_hbm, inner_high_ref), (inner_low_hbm, inner_low_ref),
        (vx_hbm, vx_ref), (vz_hbm, vz_ref), (xx_hbm, xx_ref),
        (across_high_hbm, across_high_ref), (across_low_hbm, across_low_ref),
    )
    loads = [pltpu.make_async_copy(a, b, load_sem.at[i]) for i, (a, b) in enumerate(pairs)]
    for load in loads:
        load.start()
    for load in loads[:5]:
        load.wait()

    diagonal = lax.broadcasted_iota(jnp.int32, (32, 32), 0) == lax.broadcasted_iota(
        jnp.int32, (32, 32), 1
    )
    land = (
        jnp.sum(
            jnp.where(diagonal, jnp.broadcast_to(land_ref[...], (32, 32)), 0),
            axis=1,
            keepdims=True,
        )
        > 0
    )
    land_pair = jnp.broadcast_to(jnp.concatenate([land, land], axis=0), (64, LANES))
    side[...] = land_pair.astype(jnp.int32)

    gap = jnp.zeros((CONT, 32 - WINDOW), jnp.float32)
    grams = jnp.concatenate(
        [gland_ref[...], gap, gsea_ref[...], gap, gbottom_ref[...], gap,
         jnp.zeros((CONT, 32), jnp.float32)],
        axis=1,
    )
    folded = lax.dot_general(
        grams, bound_ref[...], (((0,), (0,)), ((), ())),
        precision=lax.Precision.HIGHEST, preferred_element_type=jnp.float32,
    )
    edge_high, edge_low = parts_of(folded)
    edge_high_out[...] = edge_high
    edge_low_out[...] = edge_low

    for load in loads[5:9]:
        load.wait()
    material = load_lines(material_ref)
    density = jnp.full(material.shape, density_ref[0], jnp.float32)
    lame = jnp.full(material.shape, lame_ref[0], jnp.float32)
    shear = jnp.full(material.shape, shear_ref[0], jnp.float32)
    for layer in range(1, LAYERS):
        chosen = material == layer
        density = jnp.where(chosen, density_ref[layer], density)
        lame = jnp.where(chosen, lame_ref[layer], lame)
        shear = jnp.where(chosen, shear_ref[layer], shear)
    light = TIME_STEP * (1.0 / density)
    coefs[0] = lame
    coefs[1] = shear

    for load in loads[9:13]:
        load.wait()
    inner_high, inner_low = inner_high_ref[...], inner_low_ref[...]
    stress_xz = load_lines(xz_ref)
    stress_zz = load_lines(zz_ref)
    depth = vertical(
        jnp.concatenate([stress_xz, stress_zz], axis=0), land_pair,
        inner_high, inner_low, edge_high, edge_low,
    )
    for load in loads[13:16]:
        load.wait()
    stress_xx = load_lines(xx_ref)
    part_vx = load_lines(vx_ref) + light * depth[:32]
    part_vz = load_lines(vz_ref) + light * depth[32:]

    packed[0] = jnp.concatenate([stress_xx, stress_xz, part_vx, part_vz], axis=0).T
    packed[1] = jnp.concatenate(
        [light] + [pltpu.roll(light, NZ - slot, 1) for slot in range(1, 4)], axis=0
    ).T
    first = 0
    for piece, rows in enumerate(PIECES):
        for holder in range(HOLDERS):
            start = ROWS * holder + first
            outgoing[piece][holder, :rows] = packed[0, start : start + rows]
            for i in range(rows // 4):
                outgoing[piece][holder, rows + i : rows + i + 1] = packed[
                    1, start + 4 * i : start + 4 * i + 1
                ]
        first += rows

    @pl.when(holding)
    def _():
        for piece, rows in enumerate(PIECES):
            incoming[piece][me, : chunk_rows(rows)] = outgoing[piece][my_slot]
        pl.semaphore_wait(barrier, HOLDERS - 1)

    @pl.when(jnp.logical_not(holding))
    def _():
        pl.semaphore_wait(barrier, HOLDERS)

    def bulk(ref, count, send_semaphore, recv_semaphore):
        return pltpu.make_async_remote_copy(
            src_ref=ref.at[pl.ds(0, count)], dst_ref=ref.at[pl.ds(0, count)],
            send_sem=send_semaphore, recv_sem=recv_semaphore, device_id={"gx": early_ones[0][0]},
        )

    landings = [
        incoming[piece].at[:, pl.ds(0, chunk_rows(rows))] for piece, rows in enumerate(PIECES)
    ]
    for piece in range(len(PIECES)):

        def send(device, slot, piece=piece):
            pltpu.make_async_remote_copy(
                src_ref=outgoing[piece].at[slot], dst_ref=landings[piece].at[me],
                send_sem=send_sem.at[piece], recv_sem=recv_sem.at[piece],
                device_id={"gx": device},
            ).start()

        each_other(late_holders, send)
        each_other(early_ones, send)
    for load in loads[16:]:
        load.wait()

    def hold(piece, rows):
        across_high, across_low = across_high_ref[...], across_low_ref[...]
        bulk(landings[piece], OWNERS - 1, send_sem.at[piece], recv_sem.at[piece]).wait_recv()
        height, block = height_of(rows), block_of(rows)
        got = incoming[piece][...].reshape(8, 4, height, LANES)
        fields = swap_blocks([got[:, k].reshape(8 * height, LANES) for k in range(4)])
        row = lax.broadcasted_iota(jnp.int32, (8 * height, LANES), 0) % height
        factor = jnp.zeros((8 * height, LANES), jnp.float32)
        for i in range(rows // 4):
            for slot in range(4):
                target = 4 * i + slot
                moved = pltpu.roll(fields[slot], 8 * height + target - (rows + i), 0)
                factor = jnp.where(row == target, moved, factor)
        fields, factor = [
            [f.reshape(8, height, LANES)[:, :block].reshape(8 * block, LANES) for f in part]
            for part in (fields, [factor])
        ]
        slope = lateral(fields[:2], across_high, across_low)
        moved_vx = fields[2] + factor[0] * slope[0]
        moved_vz = fields[3] + factor[0] * slope[1]
        slope = lateral([moved_vx, moved_vz], across_high, across_low)
        result = swap_blocks([moved_vx, moved_vz, slope[0], slope[1]])
        for k in range(4):
            for part in range(8):
                returned[piece][4 * part + k] = result[k][block * part : block * part + rows]
        home[piece][my_slot] = returned[piece][me]

        def send(device, slot):
            pltpu.make_async_remote_copy(
                src_ref=returned[piece].at[device], dst_ref=home[piece].at[my_slot],
                send_sem=send_back_sem.at[piece], recv_sem=recv_back_sem.at[piece],
                device_id={"gx": device},
            ).start()

        each_other(early_ones, send)
        each_other(late_ones, send)

    @pl.when(holding)
    def _():
        for piece, rows in enumerate(PIECES):
            hold(piece, rows)

    def settle(count):
        for piece in range(len(PIECES)):
            bulk(home[piece], count, send_back_sem.at[piece], recv_back_sem.at[piece]).wait_recv()
        for piece in range(len(PIECES)):
            bulk(outgoing[piece], count, send_sem.at[piece], recv_sem.at[piece]).wait_send()

    @pl.when(holding)
    def _():
        settle(HOLDERS - 1)
        for piece in range(len(PIECES)):
            bulk(returned[piece], OWNERS - 1, send_back_sem.at[piece], recv_back_sem.at[piece]).wait_send()

    @pl.when(jnp.logical_not(holding))
    def _():
        settle(HOLDERS)


def last_kernel(*refs):
    n = len(PIECES)
    home, refs = refs[:n], refs[n:]
    (
    coefs, side, edge_high_ref, edge_low_ref, inner_high_ref, inner_low_ref,
    xx_ref, zz_ref, xz_ref,
    vx_out, vz_out, xx_out, zz_out, xz_out,
    packed,
    ) = refs
    first = 0
    for piece, rows in enumerate(PIECES):
        for holder in range(HOLDERS):
            start = ROWS * holder + first
            packed[start : start + rows] = home[piece][holder]
        first += rows
    settled = packed[...].T
    next_vx, next_vz = settled[:32], settled[32:64]
    store_lines(vx_out, next_vx)
    store_lines(vz_out, next_vz)
    lateral_vx, lateral_vz = settled[64:96], settled[96:]
    land = side[...] > 0
    depth = vertical(
        settled[:64], land, inner_high_ref[...], inner_low_ref[...],
        edge_high_ref[...], edge_low_ref[...],
    )
    depth_vx, depth_vz = depth[:32], depth[32:]
    lame, shear = coefs[0], coefs[1]
    normal = lame + 2.0 * shear
    surface = lax.broadcasted_iota(jnp.int32, (32, NZ), 1) == 0
    next_xx = load_lines(xx_ref) + TIME_STEP * (normal * lateral_vx + lame * depth_vz)
    next_zz = load_lines(zz_ref) + TIME_STEP * (lame * lateral_vx + normal * depth_vz)
    next_xz = load_lines(xz_ref) + TIME_STEP * shear * (depth_vx + lateral_vz)
    on_land = jnp.concatenate([land[:32]] * TILES, axis=1)
    next_zz = jnp.where(surface & on_land, 0.0, next_zz)
    next_xz = jnp.where(surface, 0.0, next_xz)
    store_lines(xx_out, next_xx)
    store_lines(zz_out, next_zz)
    store_lines(xz_out, next_xz)


def body(
    velocity_x, velocity_z, stress_xx, stress_zz, stress_xz, material, land_mask,
    density, lame_lambda, shear_modulus, continuation_land, continuation_sea, continuation_bottom,
):
    across = spectral(NX)
    depth = spectral(NZ + CONT)
    across_high, across_low = two_parts(across[:, :256].T)
    inner_high, inner_low = two_parts(depth[:NZ, :NZ].T)
    bound = depth[:NZ, NZ:].T.astype(np.float32)

    flat = [
        a.reshape(32 * TILES, LANES)
        for a in (velocity_x, velocity_z, stress_xx, stress_zz, stress_xz, material)
    ]
    vmem = pl.BlockSpec(memory_space=pltpu.VMEM)
    hbm = pl.BlockSpec(memory_space=pltpu.HBM)
    lines = pltpu.VMEM((32 * TILES, LANES), jnp.float32)
    square = pltpu.VMEM((NZ, NZ), jnp.bfloat16)
    edge = pltpu.VMEM((LANES, NZ), jnp.bfloat16)
    gram = pltpu.VMEM((CONT, WINDOW), jnp.float32)
    layers = pltpu.SMEM((LAYERS,), jnp.float32)
    kept = pl.pallas_call(
        kernel,
        out_shape=[
            *[pltpu.VMEM((HOLDERS, rows, LANES), jnp.float32) for rows in PIECES],
            pltpu.VMEM((2, 32, NZ), jnp.float32),
            pltpu.VMEM((64, LANES), jnp.int32),
            edge, edge, square, square, lines, lines, lines,
        ],
        in_specs=[hbm] * 18,
        out_specs=[vmem] * (9 + len(PIECES)),
        scratch_shapes=[
            lines, lines,
            pltpu.VMEM((32 * TILES, LANES), jnp.int32),
            pltpu.VMEM((1, 32), jnp.int32),
            layers, layers, layers, gram, gram, gram,
            pltpu.VMEM((CONT, NZ), jnp.float32),
            pltpu.VMEM((256, NX), jnp.bfloat16),
            pltpu.VMEM((256, NX), jnp.bfloat16),
            pltpu.VMEM((2, NZ, LANES), jnp.float32),
            *[pltpu.VMEM((HOLDERS, chunk_rows(rows), LANES), jnp.float32) for rows in PIECES],
            *[pltpu.VMEM((OWNERS, height_of(rows), LANES), jnp.float32) for rows in PIECES],
            *[pltpu.VMEM((OWNERS, rows, LANES), jnp.float32) for rows in PIECES],
            pltpu.SemaphoreType.DMA((18,)),
            *[pltpu.SemaphoreType.DMA((len(PIECES),))] * 4,
        ],
        compiler_params=pltpu.CompilerParams(
            collective_id=0, has_side_effects=True, vmem_limit_bytes=VMEM_KIB * 1024
        ),
    )(
        *flat, land_mask.reshape(1, 32), density, lame_lambda, shear_modulus,
        continuation_land, continuation_sea, continuation_bottom, jnp.asarray(bound),
        jnp.asarray(inner_high), jnp.asarray(inner_low),
        jnp.asarray(across_high), jnp.asarray(across_low),
    )
    outs = pl.pallas_call(
        last_kernel,
        out_shape=[jax.ShapeDtypeStruct((32 * TILES, LANES), jnp.float32)] * 5,
        in_specs=[vmem] * (9 + len(PIECES)),
        out_specs=[vmem] * 5,
        scratch_shapes=[pltpu.VMEM((NZ, LANES), jnp.float32)],
        compiler_params=pltpu.CompilerParams(vmem_limit_bytes=8 * 2**20),
    )(*kept)
    return tuple(a.reshape(32, 1, NZ) for a in outs)


def solution(mesh):
    split = P("gx", "gy", None)
    return jax.shard_map(
        body,
        mesh=mesh,
        in_specs=(split,) * 6 + (P("gx", "gy"),) + (P(),) * 6,
        out_specs=(split,) * 5,
        check_vma=False,
    )
```

```python
import functools

import jax
import jax.numpy as jnp
import numpy as np
from jax import lax
from jax.experimental import pallas as pl
from jax.experimental.pallas import tpu as pltpu
from jax.sharding import PartitionSpec as P

NX = 1024
NZ = 384
LAYERS = 16
WINDOW = 27
CONT = 26
RING_X = 4
RING_Z = 8
OWNERS = 32
HALF = RING_Z // 2
LATE_X = 2
HOLDERS = RING_X * HALF + LATE_X * HALF
ROWS = NZ // HOLDERS
LANES = 128
TILES = 3
TIME_STEP = 0.2
VMEM_KIB = 63900
PIECES = (4, 4, 8)


def chunk_rows(rows):
    return rows + rows // 4


def height_of(rows):
    return -(-chunk_rows(rows) // 8) * 8


def block_of(rows):
    return max(rows, 8)


def spectral(length):
    indices = np.arange(length)
    distance = np.mod(indices[:, None] - indices[None, :] + length // 2, length) - length // 2
    parity = 1.0 - 2.0 * np.mod(distance, 2)
    tangent = np.tan(np.pi * np.where(distance == 0, 1, distance) / length)
    return np.where(distance == 0, 0.0, parity * (np.pi / length) / tangent)


def two_parts(matrix):
    high = matrix.astype(np.float32).astype(jnp.bfloat16)
    low = (matrix.astype(np.float32) - high.astype(np.float32)).astype(jnp.bfloat16)
    return high, low


def parts_of(value):
    high = value.astype(jnp.bfloat16)
    low = (value - high.astype(jnp.float32)).astype(jnp.bfloat16)
    return high, low


def dot(left, right):
    return jnp.dot(left, right, preferred_element_type=jnp.float32)


def split_product(left, right_high, right_low):
    rows = left.shape[0]
    high, low = parts_of(left)
    both = dot(jnp.concatenate([high, low], axis=0), right_high)
    return both[:rows] + (both[rows:] + dot(high, right_low))


def swap_blocks(arrays):
    lane = lax.broadcasted_iota(jnp.int32, arrays[0].shape, 1)
    out = list(arrays)
    for bit, width in ((1, 32), (2, 64)):
        upper = (lane & width) != 0
        for k in range(4):
            if k & bit:
                continue
            first, second = out[k], out[k | bit]
            out[k] = jnp.where(upper, pltpu.roll(second, width, 1), first)
            out[k | bit] = jnp.where(upper, second, pltpu.roll(first, LANES - width, 1))
    return out


def lateral(fields, across_high, across_low):
    height = fields[0].shape[0] // 8
    pairs = []
    for field in fields:
        blocks = field.reshape(4, 2, height, LANES)
        pairs.append(
            jnp.concatenate(
                [blocks[:, half].reshape(4 * height, LANES) for half in range(2)], axis=1
            )
        )
    spread = split_product(jnp.concatenate(pairs, axis=0), across_high, across_low)
    results = []
    for f in range(len(fields)):
        pieces = []
        for target in range(4):
            total = None
            for source in range(4):
                shift = (target - source) % 4
                row = height * (4 * f + source)
                term = spread[row : row + height, 256 * shift : 256 * shift + 256]
                total = term if total is None else total + term
            pieces += [total[:, :LANES], total[:, LANES:]]
        results.append(jnp.concatenate(pieces, axis=0))
    return results


def vertical(lines, land, inner_high, inner_low, edge_high, edge_low):
    lane = lax.broadcasted_iota(jnp.int32, (lines.shape[0], LANES), 1)
    upper = jnp.where(lane < WINDOW, lines[:, :LANES], 0.0)
    lower = jnp.where(lane >= LANES - WINDOW, lines[:, NZ - LANES :], 0.0)
    edges = (
        jnp.where(land, upper, 0.0)
        + pltpu.roll(jnp.where(land, 0.0, upper), 32, 1)
        + pltpu.roll(lower, 64 + WINDOW, 1)
    )
    return split_product(lines, inner_high, inner_low) + split_product(edges, edge_high, edge_low)


def load_lines(ref):
    return jnp.concatenate([ref[pl.ds(t, 32, stride=TILES), :] for t in range(TILES)], axis=1)


def store_lines(ref, value):
    for t in range(TILES):
        ref[pl.ds(t, 32, stride=TILES), :] = value[:, LANES * t : LANES * (t + 1)]


def kernel(
    vx_hbm, vz_hbm, xx_hbm, zz_hbm, xz_hbm, material_hbm,
    land_hbm, density_hbm, lame_hbm, shear_hbm, gland_hbm, gsea_hbm, gbottom_hbm, bound_hbm,
    inner_high_hbm, inner_low_hbm, across_high_hbm, across_low_hbm,
    *refs,
):
    n = len(PIECES)
    home, refs = refs[:n], refs[n:]
    (
    coefs, side, edge_high_out, edge_low_out, inner_high_ref, inner_low_ref,
    xx_ref, zz_ref, xz_ref,
    vx_ref, vz_ref, material_ref, land_ref, density_ref, lame_ref, shear_ref,
    gland_ref, gsea_ref, gbottom_ref, bound_ref, across_high_ref, across_low_ref,
    packed,
    ) = refs[:-5 - 3 * n]
    outgoing, incoming, returned = refs[-5 - 3 * n:-5 - 2 * n], refs[-5 - 2 * n:-5 - n], refs[-5 - n:-5]
    load_sem, send_sem, recv_sem, send_back_sem, recv_back_sem = refs[-5:]
    me = lax.axis_index("gx")
    my_x, my_z = lax.div(me, RING_Z), lax.rem(me, RING_Z)
    early = my_z < HALF
    holding = early | (my_x < LATE_X)
    my_slot = jnp.where(early, my_x * HALF + my_z, RING_X * HALF + my_x * HALF + my_z - HALF)
    any_x = [lax.rem(my_x + dx, RING_X) for dx in range(RING_X)]
    late_x = [lax.rem(my_x + dx, LATE_X) for dx in range(LATE_X)]
    half_z = [lax.rem(my_z + dz, HALF) for dz in range(HALF)]

    def group(columns, first_z, first_slot, far):
        found = []
        for x in columns[::-1] if far else columns:
            for z in half_z[::-1] if far else half_z:
                found.append((x * RING_Z + first_z + z, first_slot + x * HALF + z))
        return found

    early_ones = group(any_x, 0, 0, True)
    late_holders = group(late_x, HALF, RING_X * HALF, True)
    late_ones = group(any_x, HALF, 0, True)

    def each_other(members, act):
        for index, (device, slot) in enumerate(members):
            if index < len(members) - 1:
                act(device, slot)
            else:
                pl.when(device != me)(functools.partial(act, device, slot))

    barrier = pltpu.get_barrier_semaphore()

    def greet(device, slot):
        pl.semaphore_signal(barrier, inc=1, device_id={"gx": device})

    @pl.when(holding)
    def _():
        each_other(early_ones, greet)
        each_other(late_ones, greet)

    pairs = (
        (land_hbm, land_ref), (gland_hbm, gland_ref), (gsea_hbm, gsea_ref),
        (gbottom_hbm, gbottom_ref), (bound_hbm, bound_ref),
        (density_hbm, density_ref), (lame_hbm, lame_ref), (shear_hbm, shear_ref),
        (material_hbm, material_ref), (xz_hbm, xz_ref), (zz_hbm, zz_ref),
        (inner_high_hbm, inner_high_ref), (inner_low_hbm, inner_low_ref),
        (vx_hbm, vx_ref), (vz_hbm, vz_ref), (xx_hbm, xx_ref),
        (across_high_hbm, across_high_ref), (across_low_hbm, across_low_ref),
    )
    loads = [pltpu.make_async_copy(a, b, load_sem.at[i]) for i, (a, b) in enumerate(pairs)]
    for load in loads:
        load.start()
    for load in loads[:5]:
        load.wait()

    diagonal = lax.broadcasted_iota(jnp.int32, (32, 32), 0) == lax.broadcasted_iota(
        jnp.int32, (32, 32), 1
    )
    land = (
        jnp.sum(
            jnp.where(diagonal, jnp.broadcast_to(land_ref[...], (32, 32)), 0),
            axis=1,
            keepdims=True,
        )
        > 0
    )
    land_pair = jnp.broadcast_to(jnp.concatenate([land, land], axis=0), (64, LANES))
    side[...] = land_pair.astype(jnp.int32)

    gap = jnp.zeros((CONT, 32 - WINDOW), jnp.float32)
    grams = jnp.concatenate(
        [gland_ref[...], gap, gsea_ref[...], gap, gbottom_ref[...], gap,
         jnp.zeros((CONT, 32), jnp.float32)],
        axis=1,
    )
    folded = lax.dot_general(
        grams, bound_ref[...], (((0,), (0,)), ((), ())),
        precision=lax.Precision.HIGHEST, preferred_element_type=jnp.float32,
    )
    edge_high, edge_low = parts_of(folded)
    edge_high_out[...] = edge_high
    edge_low_out[...] = edge_low

    for load in loads[5:9]:
        load.wait()
    material = load_lines(material_ref)
    density = jnp.full(material.shape, density_ref[0], jnp.float32)
    lame = jnp.full(material.shape, lame_ref[0], jnp.float32)
    shear = jnp.full(material.shape, shear_ref[0], jnp.float32)
    for layer in range(1, LAYERS):
        chosen = material == layer
        density = jnp.where(chosen, density_ref[layer], density)
        lame = jnp.where(chosen, lame_ref[layer], lame)
        shear = jnp.where(chosen, shear_ref[layer], shear)
    light = TIME_STEP * (1.0 / density)
    coefs[0] = lame
    coefs[1] = shear

    for load in loads[9:13]:
        load.wait()
    inner_high, inner_low = inner_high_ref[...], inner_low_ref[...]
    stress_xz = load_lines(xz_ref)
    stress_zz = load_lines(zz_ref)
    depth = vertical(
        jnp.concatenate([stress_xz, stress_zz], axis=0), land_pair,
        inner_high, inner_low, edge_high, edge_low,
    )
    for load in loads[13:16]:
        load.wait()
    stress_xx = load_lines(xx_ref)
    part_vx = load_lines(vx_ref) + light * depth[:32]
    part_vz = load_lines(vz_ref) + light * depth[32:]

    packed[0] = jnp.concatenate([stress_xx, stress_xz, part_vx, part_vz], axis=0).T
    for quarter in (1, 2):
        packed[quarter] = jnp.concatenate(
            [light] + [pltpu.roll(light, NZ - quarter * slot, 1) for slot in range(1, 4)], axis=0
        ).T
    first = 0
    for piece, rows in enumerate(PIECES):
        for holder in range(HOLDERS):
            start = ROWS * holder + first
            outgoing[piece][holder, :rows] = packed[0, start : start + rows]
            quarter = rows // 4
            outgoing[piece][holder, rows:] = packed[quarter, start : start + quarter]
        first += rows

    @pl.when(holding)
    def _():
        for piece, rows in enumerate(PIECES):
            incoming[piece][me, : chunk_rows(rows)] = outgoing[piece][my_slot]
        pl.semaphore_wait(barrier, HOLDERS - 1)

    @pl.when(jnp.logical_not(holding))
    def _():
        pl.semaphore_wait(barrier, HOLDERS)

    def bulk(ref, count, send_semaphore, recv_semaphore):
        return pltpu.make_async_remote_copy(
            src_ref=ref.at[pl.ds(0, count)], dst_ref=ref.at[pl.ds(0, count)],
            send_sem=send_semaphore, recv_sem=recv_semaphore, device_id={"gx": early_ones[0][0]},
        )

    landings = [
        incoming[piece].at[:, pl.ds(0, chunk_rows(rows))] for piece, rows in enumerate(PIECES)
    ]
    def send(piece, device, slot):
        pltpu.make_async_remote_copy(
            src_ref=outgoing[piece].at[slot], dst_ref=landings[piece].at[me],
            send_sem=send_sem.at[piece], recv_sem=recv_sem.at[piece], device_id={"gx": device},
        ).start()

    def send_to(members, *pieces):
        for piece in pieces:
            each_other(members, functools.partial(send, piece))

    every = range(len(PIECES))

    @pl.when(early)
    def _():
        for piece in every:
            send_to(late_holders, piece)
            send_to(early_ones, piece)

    @pl.when(jnp.logical_not(early))
    def _():
        for piece in every:
            send_to(early_ones, piece)
            send_to(late_holders, piece)

    for load in loads[16:]:
        load.wait()

    def hold(piece, rows):
        across_high, across_low = across_high_ref[...], across_low_ref[...]
        bulk(landings[piece], OWNERS - 1, send_sem.at[piece], recv_sem.at[piece]).wait_recv()
        height, block, quarter = height_of(rows), block_of(rows), rows // 4
        got = incoming[piece][...].reshape(8, 4, height, LANES)
        tiles = [
            swap_blocks([got[:, k, a : a + 8].reshape(8 * 8, LANES) for k in range(4)])
            for a in range(0, height, 8)
        ]
        fields, lights = tiles[0], tiles[-1]
        row = lax.broadcasted_iota(jnp.int32, (8 * 8, LANES), 0) % 8
        factor = jnp.zeros((8 * 8, LANES), jnp.float32)
        for slot in range(4):
            moved = pltpu.roll(lights[slot], (64 + quarter * slot - rows % 8) % 64, 0)
            own = (row >= quarter * slot) & (row < quarter * (slot + 1))
            factor = jnp.where(own, moved, factor)
        slope = lateral(fields[:2], across_high, across_low)
        moved_vx = fields[2] + factor * slope[0]
        moved_vz = fields[3] + factor * slope[1]
        slope = lateral([moved_vx, moved_vz], across_high, across_low)
        result = swap_blocks([moved_vx, moved_vz, slope[0], slope[1]])
        for k in range(4):
            for part in range(8):
                returned[piece][4 * part + k] = result[k][block * part : block * part + rows]
        home[piece][my_slot] = returned[piece][me]

        def send(device, slot):
            pltpu.make_async_remote_copy(
                src_ref=returned[piece].at[device], dst_ref=home[piece].at[my_slot],
                send_sem=send_back_sem.at[piece], recv_sem=recv_back_sem.at[piece],
                device_id={"gx": device},
            ).start()

        each_other(early_ones, send)
        each_other(late_ones, send)

    @pl.when(holding)
    def _():
        for piece, rows in enumerate(PIECES):
            hold(piece, rows)

    def settle(count):
        for piece in range(len(PIECES)):
            bulk(home[piece], count, send_back_sem.at[piece], recv_back_sem.at[piece]).wait_recv()
        for piece in range(len(PIECES)):
            bulk(outgoing[piece], count, send_sem.at[piece], recv_sem.at[piece]).wait_send()

    @pl.when(holding)
    def _():
        settle(HOLDERS - 1)
        for piece in range(len(PIECES)):
            bulk(returned[piece], OWNERS - 1, send_back_sem.at[piece], recv_back_sem.at[piece]).wait_send()

    @pl.when(jnp.logical_not(holding))
    def _():
        settle(HOLDERS)


def last_kernel(*refs):
    n = len(PIECES)
    home, refs = refs[:n], refs[n:]
    (
    coefs, side, edge_high_ref, edge_low_ref, inner_high_ref, inner_low_ref,
    xx_ref, zz_ref, xz_ref,
    vx_out, vz_out, xx_out, zz_out, xz_out,
    packed,
    ) = refs
    first = 0
    for piece, rows in enumerate(PIECES):
        for holder in range(HOLDERS):
            start = ROWS * holder + first
            packed[start : start + rows] = home[piece][holder]
        first += rows
    settled = packed[...].T
    next_vx, next_vz = settled[:32], settled[32:64]
    store_lines(vx_out, next_vx)
    store_lines(vz_out, next_vz)
    lateral_vx, lateral_vz = settled[64:96], settled[96:]
    land = side[...] > 0
    depth = vertical(
        settled[:64], land, inner_high_ref[...], inner_low_ref[...],
        edge_high_ref[...], edge_low_ref[...],
    )
    depth_vx, depth_vz = depth[:32], depth[32:]
    lame, shear = coefs[0], coefs[1]
    normal = lame + 2.0 * shear
    surface = lax.broadcasted_iota(jnp.int32, (32, NZ), 1) == 0
    next_xx = load_lines(xx_ref) + TIME_STEP * (normal * lateral_vx + lame * depth_vz)
    next_zz = load_lines(zz_ref) + TIME_STEP * (lame * lateral_vx + normal * depth_vz)
    next_xz = load_lines(xz_ref) + TIME_STEP * shear * (depth_vx + lateral_vz)
    on_land = jnp.concatenate([land[:32]] * TILES, axis=1)
    next_zz = jnp.where(surface & on_land, 0.0, next_zz)
    next_xz = jnp.where(surface, 0.0, next_xz)
    store_lines(xx_out, next_xx)
    store_lines(zz_out, next_zz)
    store_lines(xz_out, next_xz)


def body(
    velocity_x, velocity_z, stress_xx, stress_zz, stress_xz, material, land_mask,
    density, lame_lambda, shear_modulus, continuation_land, continuation_sea, continuation_bottom,
):
    across = spectral(NX)
    depth = spectral(NZ + CONT)
    across_high, across_low = two_parts(across[:, :256].T)
    inner_high, inner_low = two_parts(depth[:NZ, :NZ].T)
    bound = depth[:NZ, NZ:].T.astype(np.float32)

    flat = [
        a.reshape(32 * TILES, LANES)
        for a in (velocity_x, velocity_z, stress_xx, stress_zz, stress_xz, material)
    ]
    vmem = pl.BlockSpec(memory_space=pltpu.VMEM)
    hbm = pl.BlockSpec(memory_space=pltpu.HBM)
    lines = pltpu.VMEM((32 * TILES, LANES), jnp.float32)
    square = pltpu.VMEM((NZ, NZ), jnp.bfloat16)
    edge = pltpu.VMEM((LANES, NZ), jnp.bfloat16)
    gram = pltpu.VMEM((CONT, WINDOW), jnp.float32)
    layers = pltpu.SMEM((LAYERS,), jnp.float32)
    kept = pl.pallas_call(
        kernel,
        out_shape=[
            *[pltpu.VMEM((HOLDERS, rows, LANES), jnp.float32) for rows in PIECES],
            pltpu.VMEM((2, 32, NZ), jnp.float32),
            pltpu.VMEM((64, LANES), jnp.int32),
            edge, edge, square, square, lines, lines, lines,
        ],
        in_specs=[hbm] * 18,
        out_specs=[vmem] * (9 + len(PIECES)),
        scratch_shapes=[
            lines, lines,
            pltpu.VMEM((32 * TILES, LANES), jnp.int32),
            pltpu.VMEM((1, 32), jnp.int32),
            layers, layers, layers, gram, gram, gram,
            pltpu.VMEM((CONT, NZ), jnp.float32),
            pltpu.VMEM((256, NX), jnp.bfloat16),
            pltpu.VMEM((256, NX), jnp.bfloat16),
            pltpu.VMEM((3, NZ, LANES), jnp.float32),
            *[pltpu.VMEM((HOLDERS, chunk_rows(rows), LANES), jnp.float32) for rows in PIECES],
            *[pltpu.VMEM((OWNERS, height_of(rows), LANES), jnp.float32) for rows in PIECES],
            *[pltpu.VMEM((OWNERS, rows, LANES), jnp.float32) for rows in PIECES],
            pltpu.SemaphoreType.DMA((18,)),
            *[pltpu.SemaphoreType.DMA((len(PIECES),))] * 4,
        ],
        compiler_params=pltpu.CompilerParams(
            collective_id=0, has_side_effects=True, vmem_limit_bytes=VMEM_KIB * 1024
        ),
    )(
        *flat, land_mask.reshape(1, 32), density, lame_lambda, shear_modulus,
        continuation_land, continuation_sea, continuation_bottom, jnp.asarray(bound),
        jnp.asarray(inner_high), jnp.asarray(inner_low),
        jnp.asarray(across_high), jnp.asarray(across_low),
    )
    outs = pl.pallas_call(
        last_kernel,
        out_shape=[jax.ShapeDtypeStruct((32 * TILES, LANES), jnp.float32)] * 5,
        in_specs=[vmem] * (9 + len(PIECES)),
        out_specs=[vmem] * 5,
        scratch_shapes=[pltpu.VMEM((NZ, LANES), jnp.float32)],
        compiler_params=pltpu.CompilerParams(vmem_limit_bytes=8 * 2**20),
    )(*kept)
    return tuple(a.reshape(32, 1, NZ) for a in outs)


def solution(mesh):
    split = P("gx", "gy", None)
    return jax.shard_map(
        body,
        mesh=mesh,
        in_specs=(split,) * 6 + (P("gx", "gy"),) + (P(),) * 6,
        out_specs=(split,) * 5,
        check_vma=False,
    )
```
